32 devices in a mesh: dp: 4 (over y, z), cp: 8 (over x, core).
Axes of the slice: x: 4, y: 2, z: 2, core: 2. Of those that a mesh axis runs over, the one named last changes fastest.
The devices are a block of a 4x4x8 slice.
Arguments:
- x_in: bfloat16 [32, 2048, 1152], P('dp', 'cp'), parts along dimension 0
- positions: int32 [32, 2048], P('dp', 'cp'), parts along dimension 0
- dy_out: bfloat16 [32, 2048, 1152], P('dp', 'cp'), parts along dimension 0
- w_query: bfloat16 [1152, 4, 256], replicated
- w_key: bfloat16 [1152, 1, 256], replicated
- w_value: bfloat16 [1152, 1, 256], replicated
- w_out: bfloat16 [4, 256, 1152], replicated
- w_pre: float32 [1152], replicated
- w_post: float32 [1152], replicated
Outputs:
- output 1: bfloat16 [32, 2048, 1152], P('dp', 'cp'), parts along dimension 0
- output 2: bfloat16 [32, 2048, 1152], P('dp', 'cp'), parts along dimension 0
- output 3: float32 [4608, 4, 256], P('dp'), parts along dimension 0
- output 4: float32 [4608, 1, 256], P('dp'), parts along dimension 0
- output 5: float32 [4608, 1, 256], P('dp'), parts along dimension 0
- output 6: float32 [16, 256, 1152], P('dp'), parts along dimension 0
- output 7: float32 [4608], P('dp'), parts along dimension 0
- output 8: float32 [4608], P('dp'), parts along dimension 0
There are 4 independent parts. The reference program is written for one: setup_inputs(seed, part) draws one part's arguments, and reference() takes and returns one part's arrays. A program takes and returns all parts, laid end to end along the dimension named above; an argument that names none is the same for every part.
All inputs are finite; a program needn't handle non-finite values.
Results may differ from the reference program's by a relative error of at most 0.02.
Values are sent between devices in bfloat16 or wider.
A program may use at most 768 MiB of HBM per device.

```python
import jax
import jax.numpy as jnp
from jax import lax

BATCH = 8
SEQ_LEN = 2048
QUERY_BLOCK = 256
MODEL_DIM = 1152
HEADS = 4
KV_HEADS = 1
HEAD_DIM = 256

NORM_EPS = 1e-6
SOFT_CAP = 50.0
QUERY_SCALE = 144.0
ROPE_BASE = 10000.0


def rms_scale(values, gain):
    return values * lax.rsqrt(jnp.mean(values * values, axis=-1, keepdims=True) + NORM_EPS) * (1.0 + gain)


def rope_tables(positions):
    half = HEAD_DIM // 2
    inv_freq = ROPE_BASE ** (jnp.arange(half, dtype=jnp.float32) * (-2.0 / HEAD_DIM))
    angles = positions.astype(jnp.float32)[:, :, None, None] * inv_freq
    return jnp.cos(angles), jnp.sin(angles)


def rotate(values, cosine, sine):
    half = values.shape[-1] // 2
    first = values[..., :half]
    second = values[..., half:]
    return jnp.concatenate([first * cosine - second * sine, second * cosine + first * sine], axis=-1)


def rotate_back(values, cosine, sine):
    half = values.shape[-1] // 2
    first = values[..., :half]
    second = values[..., half:]
    return jnp.concatenate([first * cosine + second * sine, second * cosine - first * sine], axis=-1)


def setup_inputs(seed: int = 0, part: int = 0) -> dict:
    base = jax.random.key(seed)
    shared = jax.random.split(base, 6)
    local = jax.random.split(jax.random.fold_in(base, part), 4)
    in_scale = MODEL_DIM ** -0.5
    x_in = jax.random.normal(local[0], (BATCH, SEQ_LEN, MODEL_DIM), jnp.float32).astype(jnp.bfloat16)
    start = jax.random.randint(local[1], (BATCH, 1), 0, SEQ_LEN, dtype=jnp.int32)
    steps = jax.random.randint(local[2], (BATCH, SEQ_LEN), 1, 4, dtype=jnp.int32)
    positions = start + jnp.cumsum(steps, axis=1) - steps[:, :1]
    dy_out = jax.random.normal(local[3], (BATCH, SEQ_LEN, MODEL_DIM), jnp.float32).astype(jnp.bfloat16)
    w_query = (jax.random.normal(shared[0], (MODEL_DIM, HEADS, HEAD_DIM), jnp.float32) * (1.5 * in_scale)).astype(jnp.bfloat16)
    w_key = (jax.random.normal(shared[1], (MODEL_DIM, KV_HEADS, HEAD_DIM), jnp.float32) * (1.5 * in_scale)).astype(jnp.bfloat16)
    w_value = (jax.random.normal(shared[2], (MODEL_DIM, KV_HEADS, HEAD_DIM), jnp.float32) * in_scale).astype(jnp.bfloat16)
    w_out = (jax.random.normal(shared[3], (HEADS, HEAD_DIM, MODEL_DIM), jnp.float32) * (HEADS * HEAD_DIM) ** -0.5).astype(jnp.bfloat16)
    w_pre = 0.3 * jax.random.normal(shared[4], (MODEL_DIM,), jnp.float32)
    w_post = 0.3 * jax.random.normal(shared[5], (MODEL_DIM,), jnp.float32)
    return {"x_in": x_in, "positions": positions, "dy_out": dy_out, "w_query": w_query, "w_key": w_key, "w_value": w_value, "w_out": w_out, "w_pre": w_pre, "w_post": w_post}


def reference(x_in, positions, dy_out, w_query, w_key, w_value, w_out, w_pre, w_post):
    group = HEADS // KV_HEADS
    tokens = BATCH * SEQ_LEN
    blocks = SEQ_LEN // QUERY_BLOCK
    width_q = HEADS * HEAD_DIM
    width_kv = KV_HEADS * HEAD_DIM
    wq_flat = w_query.reshape(MODEL_DIM, width_q)
    wk_flat = w_key.reshape(MODEL_DIM, width_kv)
    wv_flat = w_value.reshape(MODEL_DIM, width_kv)
    wo_flat = w_out.reshape(width_q, MODEL_DIM)
    x_float = x_in.astype(jnp.float32).reshape(tokens, MODEL_DIM)
    normed, pre_vjp = jax.vjp(rms_scale, x_float, w_pre)
    act_flat = normed.astype(jnp.bfloat16)
    query_proj = jnp.dot(act_flat, wq_flat, preferred_element_type=jnp.float32).astype(jnp.bfloat16)
    key_proj = jnp.dot(act_flat, wk_flat, preferred_element_type=jnp.float32).astype(jnp.bfloat16)
    value_proj = jnp.dot(act_flat, wv_flat, preferred_element_type=jnp.float32).astype(jnp.bfloat16)
    cosine, sine = rope_tables(positions)
    query_rot = (rotate(query_proj.astype(jnp.float32).reshape(BATCH, SEQ_LEN, HEADS, HEAD_DIM), cosine, sine) * QUERY_SCALE ** -0.5).astype(jnp.bfloat16)
    key_rot = rotate(key_proj.astype(jnp.float32).reshape(BATCH, SEQ_LEN, KV_HEADS, HEAD_DIM), cosine, sine).astype(jnp.bfloat16)
    key_float = key_rot.astype(jnp.float32)
    value_float = value_proj.reshape(BATCH, SEQ_LEN, KV_HEADS, HEAD_DIM).astype(jnp.float32)

    def to_blocks(arr):
        moved = arr.reshape((BATCH, blocks, QUERY_BLOCK) + arr.shape[2:])
        return jnp.moveaxis(moved, 1, 0)

    def from_blocks(arr):
        return jnp.moveaxis(arr, 0, 1).reshape((BATCH, SEQ_LEN) + arr.shape[3:])

    query_blocks = to_blocks(query_rot.reshape(BATCH, SEQ_LEN, KV_HEADS, group, HEAD_DIM))
    pos_blocks = to_blocks(positions)

    def block_probs(query_blk, pos_blk):
        scores = jnp.einsum("bqngd,bknd->bnqgk", query_blk.astype(jnp.float32), key_float)
        capped = SOFT_CAP * jnp.tanh(scores / SOFT_CAP)
        allowed = positions[:, None, None, None, :] <= pos_blk[:, None, :, None, None]
        soft_probs = jax.nn.softmax(jnp.where(allowed, capped, -1e30), axis=-1)
        return soft_probs, capped

    def forward_block(pair):
        soft_probs, capped = block_probs(pair[0], pair[1])
        return jnp.einsum("bnqgk,bknd->bqngd", soft_probs.astype(jnp.bfloat16).astype(jnp.float32), value_float)

    attn_float = from_blocks(lax.map(forward_block, (query_blocks, pos_blocks)))
    attn_flat = attn_float.astype(jnp.bfloat16).reshape(tokens, width_q)
    z_out = jnp.dot(attn_flat, wo_flat, preferred_element_type=jnp.float32).astype(jnp.bfloat16)
    post_normed, post_vjp = jax.vjp(rms_scale, z_out.astype(jnp.float32), w_post)
    y_out = (x_float + post_normed.astype(jnp.bfloat16).astype(jnp.float32)).astype(jnp.bfloat16)

    dy_float = dy_out.astype(jnp.float32).reshape(tokens, MODEL_DIM)
    dz_float, dw_post = post_vjp(dy_float)
    dz_out = dz_float.astype(jnp.bfloat16)
    dw_out = jnp.dot(attn_flat.T, dz_out, preferred_element_type=jnp.float32)
    d_attn = jnp.dot(dz_out, wo_flat.T, preferred_element_type=jnp.float32).astype(jnp.bfloat16).reshape(BATCH, SEQ_LEN, KV_HEADS, group, HEAD_DIM)
    row_dot = jnp.sum(d_attn.astype(jnp.float32) * attn_float, axis=-1)

    def backward_block(carry, items):
        dkey_sum, dvalue_sum = carry
        query_blk, pos_blk, dattn_blk, delta_blk = items
        soft_probs, capped = block_probs(query_blk, pos_blk)
        dattn_float = dattn_blk.astype(jnp.float32)
        d_probs = jnp.einsum("bqngd,bknd->bnqgk", dattn_float, value_float)
        dvalue_sum = dvalue_sum + jnp.einsum("bnqgk,bqngd->bknd", soft_probs.astype(jnp.bfloat16).astype(jnp.float32), dattn_float)
        delta_t = jnp.moveaxis(delta_blk, 1, 2)
        d_scores = (soft_probs * (d_probs - delta_t[..., None]) * (1.0 - (capped / SOFT_CAP) ** 2)).astype(jnp.bfloat16).astype(jnp.float32)
        dquery_blk = jnp.einsum("bnqgk,bknd->bqngd", d_scores, key_float)
        dkey_sum = dkey_sum + jnp.einsum("bnqgk,bqngd->bknd", d_scores, query_blk.astype(jnp.float32))
        return (dkey_sum, dvalue_sum), dquery_blk

    kv_zeros = jnp.zeros((BATCH, SEQ_LEN, KV_HEADS, HEAD_DIM), jnp.float32)
    sums_kv, dquery_blocks = lax.scan(backward_block, (kv_zeros, kv_zeros), (query_blocks, pos_blocks, to_blocks(d_attn), to_blocks(row_dot)))
    dquery_rot = from_blocks(dquery_blocks).reshape(BATCH, SEQ_LEN, HEADS, HEAD_DIM)
    dquery = (rotate_back(dquery_rot, cosine, sine) * QUERY_SCALE ** -0.5).astype(jnp.bfloat16).reshape(tokens, width_q)
    dkey = rotate_back(sums_kv[0], cosine, sine).astype(jnp.bfloat16).reshape(tokens, width_kv)
    dvalue = sums_kv[1].astype(jnp.bfloat16).reshape(tokens, width_kv)
    dw_query = jnp.dot(act_flat.T, dquery, preferred_element_type=jnp.float32).reshape(MODEL_DIM, HEADS, HEAD_DIM)
    dw_key = jnp.dot(act_flat.T, dkey, preferred_element_type=jnp.float32).reshape(MODEL_DIM, KV_HEADS, HEAD_DIM)
    dw_value = jnp.dot(act_flat.T, dvalue, preferred_element_type=jnp.float32).reshape(MODEL_DIM, KV_HEADS, HEAD_DIM)
    d_act = (jnp.dot(dquery, wq_flat.T, preferred_element_type=jnp.float32) + jnp.dot(dkey, wk_flat.T, preferred_element_type=jnp.float32) + jnp.dot(dvalue, wv_flat.T, preferred_element_type=jnp.float32))
    dx_float, dw_pre = pre_vjp(d_act)
    dx_in = (dy_float + dx_float).astype(jnp.bfloat16).reshape(BATCH, SEQ_LEN, MODEL_DIM)
    return (y_out.reshape(BATCH, SEQ_LEN, MODEL_DIM), dx_in, dw_query, dw_key, dw_value, dw_out.reshape(HEADS, HEAD_DIM, MODEL_DIM), dw_pre, dw_post)
```

```python
import functools

import jax
import jax.numpy as jnp
from jax import lax
from jax.experimental import pallas as pl
from jax.experimental.pallas import tpu as pltpu
from jax.sharding import PartitionSpec as P

NORM_EPS = 1e-6
SOFT_CAP = 50.0
QUERY_SCALE = 144.0
ROPE_BASE = 10000.0

NN = (((1,), (0,)), ((), ()))
NT = (((1,), (1,)), ((), ()))
TN = (((0,), (0,)), ((), ()))


def dot(a, b, dims=NN):
    return lax.dot_general(a, b, dims, preferred_element_type=jnp.float32)


def rope_tables(positions, head_dim):
    half = head_dim // 2
    inv_freq = ROPE_BASE ** (jnp.arange(half, dtype=jnp.float32) * (-2.0 / head_dim))
    angles = positions.astype(jnp.float32)[:, :, None] * inv_freq
    return jnp.cos(angles), jnp.sin(angles)


def rotate(values, cosine, sine):
    half = values.shape[-1] // 2
    first = values[..., :half]
    second = values[..., half:]
    return jnp.concatenate([first * cosine - second * sine, second * cosine + first * sine], axis=-1)


def rotate_back(values, cosine, sine):
    half = values.shape[-1] // 2
    first = values[..., :half]
    second = values[..., half:]
    return jnp.concatenate([first * cosine + second * sine, second * cosine - first * sine], axis=-1)


def bf(values):
    return values.astype(jnp.bfloat16)


def inv_rms(values):
    return lax.rsqrt(jnp.mean(values * values, axis=-1, keepdims=True) + NORM_EPS)


def pre_kernel(heads, x_ref, cos_ref, sin_ref, gain_ref, wq_ref, wk_ref, wv_ref, act_ref, q_ref, k_ref, kt_ref, v_ref, vt_ref):
    x = x_ref[0].astype(jnp.float32)
    act = bf(x * inv_rms(x) * (1.0 + gain_ref[...]))
    act_ref[0] = act
    cosine, sine = cos_ref[0], sin_ref[0]
    dim = k_ref.shape[-1]
    for h in range(heads):
        cols = slice(h * dim, (h + 1) * dim)
        qh = bf(dot(act, wq_ref[:, cols])).astype(jnp.float32)
        q_ref[0, :, cols] = bf(rotate(qh, cosine, sine) * QUERY_SCALE ** -0.5)
    kh = rotate(bf(dot(act, wk_ref[...])).astype(jnp.float32), cosine, sine)
    k_ref[0] = bf(kh)
    kt_ref[0] = bf(kh.T)
    vh = dot(act, wv_ref[...])
    v_ref[0] = bf(vh)
    vt_ref[0] = bf(vh.T)


def fwd_kernel(heads, q_ref, k_ref, vt_ref, wo_ref, x_ref, gain_ref, of_ref, o_ref, z_ref, y_ref, lse_ref, acc_ref, stat_ref):
    i = pl.program_id(0)
    rows, dim = q_ref.shape[1], k_ref.shape[-1]
    acc_ref[...] = jnp.zeros_like(acc_ref)
    stat_ref[0] = jnp.full(stat_ref.shape[1:], -1e30, jnp.float32)
    stat_ref[1] = jnp.zeros(stat_ref.shape[1:], jnp.float32)

    def block(j, masked):
        key = k_ref[j]
        val_t = vt_ref[j]
        for h in range(heads):
            s = dot(key, q_ref[0, :, h * dim:(h + 1) * dim], NT)
            c = SOFT_CAP * jnp.tanh(s * (1.0 / SOFT_CAP))
            if masked:
                allowed = lax.broadcasted_iota(jnp.int32, s.shape, 0) <= lax.broadcasted_iota(jnp.int32, s.shape, 1)
                c = jnp.where(allowed, c, -1e30)
            old = stat_ref[0, h:h + 1, :]
            new = jnp.maximum(old, jnp.max(c, axis=0, keepdims=True))
            scale = jnp.exp(old - new)
            p = jnp.exp(c - new)
            stat_ref[1, h:h + 1, :] = stat_ref[1, h:h + 1, :] * scale + jnp.sum(p, axis=0, keepdims=True)
            stat_ref[0, h:h + 1, :] = new
            acc_ref[h] = acc_ref[h] * scale + dot(val_t, bf(p))

    def body(j, carry):
        block(j, False)
        return carry

    lax.fori_loop(0, i, body, 0)
    block(i, True)
    lse_ref[0] = stat_ref[0] + jnp.log(stat_ref[1])
    z = jnp.zeros((rows, wo_ref.shape[-1]), jnp.float32)
    for h in range(heads):
        out = (acc_ref[h] / stat_ref[1, h:h + 1, :]).T
        of_ref[0, :, h * dim:(h + 1) * dim] = out
        o_ref[0, :, h * dim:(h + 1) * dim] = bf(out)
    z = bf(dot(o_ref[0], wo_ref[...]))
    z_ref[0] = z
    zf = z.astype(jnp.float32)
    post = bf(zf * inv_rms(zf) * (1.0 + gain_ref[...]))
    y_ref[0] = bf(x_ref[0].astype(jnp.float32) + post.astype(jnp.float32))


def norm_grad(u, gain, cot):
    r = inv_rms(u)
    g = cot * (1.0 + gain)
    du = r * g - u * (r * r * r) * jnp.mean(g * u, axis=-1, keepdims=True)
    return du, cot * (u * r)


def fold_rows(values, ref):
    part = jnp.sum(values.reshape(values.shape[0] // 8, 8, values.shape[1]), axis=0)

    @pl.when(pl.program_id(0) == 0)
    def _():
        ref[...] = part

    @pl.when(pl.program_id(0) != 0)
    def _():
        ref[...] += part


def mid_kernel(heads, dy_ref, z_ref, of_ref, wo_ref, gain_ref, dz_ref, do_ref, delta_ref, dgain_ref):
    rows = dy_ref.shape[1]
    dim = of_ref.shape[-1] // heads
    dz, dgain = norm_grad(z_ref[0].astype(jnp.float32), gain_ref[...], dy_ref[0].astype(jnp.float32))
    fold_rows(dgain, dgain_ref)
    dz = bf(dz)
    dz_ref[0] = dz
    lane = lax.broadcasted_iota(jnp.int32, (rows, 128), 1)
    cols = jnp.zeros((rows, 128), jnp.float32)
    for h in range(heads):
        sl = slice(h * dim, (h + 1) * dim)
        do = bf(dot(dz, wo_ref[sl, :], NT))
        do_ref[0, :, sl] = do
        cols = jnp.where(lane == h, jnp.sum(do.astype(jnp.float32) * of_ref[0, :, sl], axis=-1, keepdims=True), cols)
    delta_ref[0] = cols.T[:8, :]


def bwd_kernel(heads, q_ref, do_ref, lse_ref, delta_ref, cos_ref, sin_ref, k_ref, kt_ref, v_ref, dq_ref, dk_ref, dv_ref, dqt_ref, dka_ref, dva_ref):
    i = pl.num_programs(0) - 1 - pl.program_id(0)
    dim = k_ref.shape[-1]

    @pl.when(pl.program_id(0) == 0)
    def _():
        dka_ref[...] = jnp.zeros_like(dka_ref)
        dva_ref[...] = jnp.zeros_like(dva_ref)

    dqt_ref[...] = jnp.zeros_like(dqt_ref)

    def block(j, masked):
        key, key_t, val = k_ref[j], kt_ref[j], v_ref[j]
        for h in range(heads):
            qh = q_ref[0, :, h * dim:(h + 1) * dim]
            doh = do_ref[0, :, h * dim:(h + 1) * dim]
            t = jnp.tanh(dot(key, qh, NT) * (1.0 / SOFT_CAP))
            p = jnp.exp(SOFT_CAP * t - lse_ref[0, h:h + 1, :])
            if masked:
                allowed = lax.broadcasted_iota(jnp.int32, t.shape, 0) <= lax.broadcasted_iota(jnp.int32, t.shape, 1)
                p = jnp.where(allowed, p, 0.0)
            dp = dot(val, doh, NT)
            ds = bf(p * (dp - delta_ref[0, h:h + 1, :]) * (1.0 - t * t))
            dva_ref[j] += dot(bf(p), doh)
            dka_ref[j] += dot(ds, qh)
            dqt_ref[h] += dot(key_t, ds)

    def body(j, carry):
        block(j, False)
        return carry

    lax.fori_loop(0, i, body, 0)
    block(i, True)
    cosine, sine = cos_ref[0], sin_ref[0]
    for h in range(heads):
        dq_ref[0, :, h * dim:(h + 1) * dim] = bf(rotate_back(dqt_ref[h].T, cosine, sine) * QUERY_SCALE ** -0.5)
    dk_ref[0] = bf(rotate_back(dka_ref[i], cosine, sine))
    dv_ref[0] = bf(dva_ref[i])


def post_kernel(dq_ref, dk_ref, dv_ref, x_ref, dy_ref, gain_ref, wq_ref, wk_ref, wv_ref, dx_ref, dgain_ref):
    da = dot(dq_ref[0], wq_ref[...], NT) + dot(dk_ref[0], wk_ref[...], NT) + dot(dv_ref[0], wv_ref[...], NT)
    du, dgain = norm_grad(x_ref[0].astype(jnp.float32), gain_ref[...], da)
    fold_rows(dgain, dgain_ref)
    dx_ref[0] = bf(dy_ref[0].astype(jnp.float32) + du)


def piece(*shape, order=None):
    index = (lambda i: (i, 0, 0)) if order is None else (lambda i: (order - 1 - i, 0, 0))
    return pl.BlockSpec((1,) + shape, index)


def whole(*shape):
    zeros = (0,) * len(shape)
    return pl.BlockSpec(shape, lambda i: zeros)


def call(kernel, name, pieces, in_specs, outs, scratch, flops, *args):
    return pl.pallas_call(
        kernel,
        name=name,
        grid=(pieces,),
        in_specs=in_specs,
        out_specs=[spec for spec, _, _ in outs],
        out_shape=[jax.ShapeDtypeStruct(shape, dtype) for _, shape, dtype in outs],
        scratch_shapes=scratch,
        compiler_params=pltpu.CompilerParams(dimension_semantics=("arbitrary",), vmem_limit_bytes=60000 * 1024),
        cost_estimate=pl.CostEstimate(flops=flops, bytes_accessed=8 * 2 ** 20, transcendentals=0),
    )(*args)


def exchange(values, count):
    me = lax.axis_index("cp")
    out = jnp.zeros_like(values)
    own = lax.dynamic_slice_in_dim(values, me, 1, 0)
    parts = [(me, own)]
    for step in (4, 3, 5, 2, 6, 7, 1):
        send = lax.dynamic_slice_in_dim(values, lax.rem(me + step, count), 1, 0)
        got = lax.ppermute(send, "cp", [(d, (d + step) % count) for d in range(count)])
        parts.append((lax.rem(me + count - step, count), got))
    for at, part in parts:
        out = lax.dynamic_update_slice_in_dim(out, part, at, 0)
    return out


def solution(mesh):
    count = mesh.shape["cp"]

    def local_step(x_in, positions, dy_out, w_query, w_key, w_value, w_out, w_pre, w_post):
        batch, rows, model = x_in.shape
        heads, dim = w_query.shape[1], w_query.shape[2]
        width = heads * dim
        pieces = count
        bf16, f32 = jnp.bfloat16, jnp.float32
        wq = w_query.reshape(model, width)
        wk = w_key.reshape(model, dim)
        wv = w_value.reshape(model, dim)
        wo = w_out.reshape(width, model)
        gain_pre = w_pre.reshape(1, model)
        gain_post = w_post.reshape(1, model)

        pos = lax.all_to_all(positions, "cp", 0, 0, tiled=True)
        x = lax.all_to_all(x_in, "cp", 0, 0, tiled=True)
        dy = exchange(dy_out, count)
        cosine, sine = rope_tables(pos, dim)

        act, q, k, kt, v, vt = call(
            functools.partial(pre_kernel, heads), "pre", pieces,
            [piece(rows, model), piece(rows, dim // 2), piece(rows, dim // 2), whole(1, model), whole(model, width), whole(model, dim), whole(model, dim)],
            [(piece(rows, model), (pieces, rows, model), bf16), (piece(rows, width), (pieces, rows, width), bf16)]
            + [(piece(rows, dim), (pieces, rows, dim), bf16)] * 4,
            [], 2 * 10 ** 9, x, cosine, sine, gain_pre, wq, wk, wv)

        of, o, z, y, lse = call(
            functools.partial(fwd_kernel, heads), "fwd", pieces,
            [piece(rows, width), whole(pieces, rows, dim), whole(pieces, dim, rows), whole(width, model), piece(rows, model), whole(1, model)],
            [(piece(rows, width), (pieces, rows, width), f32), (piece(rows, width), (pieces, rows, width), bf16),
             (piece(rows, model), (pieces, rows, model), bf16), (piece(rows, model), (pieces, rows, model), bf16),
             (piece(8, rows), (pieces, 8, rows), f32)],
            [pltpu.VMEM((heads, dim, rows), f32), pltpu.VMEM((2, 8, rows), f32)], 6 * 10 ** 9,
            q, k, vt, wo, x, gain_post)
        y_out = exchange(y, count)

        dz, do, delta, dpost = call(
            functools.partial(mid_kernel, heads), "mid", pieces,
            [piece(rows, model), piece(rows, model), piece(rows, width), whole(width, model), whole(1, model)],
            [(piece(rows, model), (pieces, rows, model), bf16), (piece(rows, width), (pieces, rows, width), bf16),
             (piece(8, rows), (pieces, 8, rows), f32), (whole(8, model), (8, model), f32)],
            [], 2 * 10 ** 9, dy, z, of, wo, gain_post)
        tokens = pieces * rows
        dwo = dot(o.reshape(tokens, width), dz.reshape(tokens, model), TN)
        dwo = lax.psum(dwo, "cp")

        dq, dk, dv = call(
            functools.partial(bwd_kernel, heads), "bwd", pieces,
            [piece(rows, width, order=pieces), piece(rows, width, order=pieces), piece(8, rows, order=pieces), piece(8, rows, order=pieces),
             piece(rows, dim // 2, order=pieces), piece(rows, dim // 2, order=pieces),
             whole(pieces, rows, dim), whole(pieces, dim, rows), whole(pieces, rows, dim)],
            [(piece(rows, width, order=pieces), (pieces, rows, width), bf16),
             (piece(rows, dim, order=pieces), (pieces, rows, dim), bf16), (piece(rows, dim, order=pieces), (pieces, rows, dim), bf16)],
            [pltpu.VMEM((heads, dim, rows), f32), pltpu.VMEM((pieces, rows, dim), f32), pltpu.VMEM((pieces, rows, dim), f32)], 12 * 10 ** 9,
            q, do, lse, delta, cosine, sine, k, kt, v)

        a_flat = act.reshape(tokens, model)
        dwq = dot(a_flat, dq.reshape(tokens, width), TN)
        dwk = dot(a_flat, dk.reshape(tokens, dim), TN)
        dwv = dot(a_flat, dv.reshape(tokens, dim), TN)
        dx, dpre = call(
            post_kernel, "post", pieces,
            [piece(rows, width), piece(rows, dim), piece(rows, dim), piece(rows, model), piece(rows, model), whole(1, model),
             whole(model, width), whole(model, dim), whole(model, dim)],
            [(piece(rows, model), (pieces, rows, model), bf16), (whole(8, model), (8, model), f32)],
            [], 2 * 10 ** 9, dq, dk, dv, x, dy, gain_pre, wq, wk, wv)
        dwq, dwk, dwv, dpre, dpost = lax.psum((dwq, dwk, dwv, jnp.sum(dpre, axis=0), jnp.sum(dpost, axis=0)), "cp")
        dx_in = exchange(dx, count)
        return (y_out, dx_in, dwq.reshape(model, heads, dim), dwk.reshape(model, 1, dim), dwv.reshape(model, 1, dim),
                dwo.reshape(heads, dim, model), dpre, dpost)

    seq_spec = P("dp", "cp", None)
    in_specs = (seq_spec, P("dp", "cp"), seq_spec, P(), P(), P(), P(), P(), P())
    out_specs = (seq_spec, seq_spec, P("dp", None, None), P("dp", None, None), P("dp", None, None), P("dp", None, None), P("dp"), P("dp"))
    return jax.shard_map(local_step, mesh=mesh, in_specs=in_specs, out_specs=out_specs, check_vma=False)
```

```python
import functools

import jax
import jax.numpy as jnp
from jax import lax
from jax.experimental import pallas as pl
from jax.experimental.pallas import tpu as pltpu
from jax.sharding import PartitionSpec as P

NORM_EPS = 1e-6
SOFT_CAP = 50.0
QUERY_SCALE = 144.0
ROPE_BASE = 10000.0

NN = (((1,), (0,)), ((), ()))
NT = (((1,), (1,)), ((), ()))
TN = (((0,), (0,)), ((), ()))


def dot(a, b, dims=NN):
    return lax.dot_general(a, b, dims, preferred_element_type=jnp.float32)


def rope_tables(positions, head_dim):
    half = head_dim // 2
    inv_freq = ROPE_BASE ** (jnp.arange(half, dtype=jnp.float32) * (-2.0 / head_dim))
    angles = positions.astype(jnp.float32)[:, :, None] * inv_freq
    return jnp.cos(angles), jnp.sin(angles)


def rotate(values, cosine, sine):
    half = values.shape[-1] // 2
    first = values[..., :half]
    second = values[..., half:]
    return jnp.concatenate([first * cosine - second * sine, second * cosine + first * sine], axis=-1)


def rotate_back(values, cosine, sine):
    half = values.shape[-1] // 2
    first = values[..., :half]
    second = values[..., half:]
    return jnp.concatenate([first * cosine + second * sine, second * cosine - first * sine], axis=-1)


def bf(values):
    return values.astype(jnp.bfloat16)


def inv_rms(values):
    return lax.rsqrt(jnp.mean(values * values, axis=-1, keepdims=True) + NORM_EPS)


def pre_kernel(heads, x_ref, cos_ref, sin_ref, gain_ref, wq_ref, wk_ref, wv_ref, act_ref, q_ref, k_ref, kt_ref, v_ref, vt_ref):
    x = x_ref[0].astype(jnp.float32)
    act = bf(x * inv_rms(x) * (1.0 + gain_ref[...]))
    act_ref[0] = act
    cosine, sine = cos_ref[0], sin_ref[0]
    dim = k_ref.shape[-1]
    for h in range(heads):
        cols = slice(h * dim, (h + 1) * dim)
        qh = bf(dot(act, wq_ref[:, cols])).astype(jnp.float32)
        q_ref[0, :, cols] = bf(rotate(qh, cosine, sine) * QUERY_SCALE ** -0.5)
    kh = rotate(bf(dot(act, wk_ref[...])).astype(jnp.float32), cosine, sine)
    k_ref[0] = bf(kh)
    kt_ref[0] = bf(kh.T)
    vh = dot(act, wv_ref[...])
    v_ref[0] = bf(vh)
    vt_ref[0] = bf(vh.T)


def fwd_kernel(heads, q_ref, k_ref, vt_ref, wo_ref, x_ref, gain_ref, of_ref, o_ref, z_ref, y_ref, lse_ref, acc_ref, stat_ref):
    i = pl.program_id(0)
    rows, dim = q_ref.shape[1], k_ref.shape[-1]
    acc_ref[...] = jnp.zeros_like(acc_ref)
    stat_ref[0] = jnp.full(stat_ref.shape[1:], -1e30, jnp.float32)
    stat_ref[1] = jnp.zeros(stat_ref.shape[1:], jnp.float32)

    def block(j, masked):
        key = k_ref[j]
        val_t = vt_ref[j]
        for h in range(heads):
            s = dot(key, q_ref[0, :, h * dim:(h + 1) * dim], NT)
            c = SOFT_CAP * jnp.tanh(s * (1.0 / SOFT_CAP))
            if masked:
                allowed = lax.broadcasted_iota(jnp.int32, s.shape, 0) <= lax.broadcasted_iota(jnp.int32, s.shape, 1)
                c = jnp.where(allowed, c, -1e30)
            old = stat_ref[0, h:h + 1, :]
            new = jnp.maximum(old, jnp.max(c, axis=0, keepdims=True))
            scale = jnp.exp(old - new)
            p = jnp.exp(c - new)
            stat_ref[1, h:h + 1, :] = stat_ref[1, h:h + 1, :] * scale + jnp.sum(p, axis=0, keepdims=True)
            stat_ref[0, h:h + 1, :] = new
            acc_ref[h] = acc_ref[h] * scale + dot(val_t, bf(p))

    def body(j, carry):
        block(j, False)
        return carry

    lax.fori_loop(0, i, body, 0)
    block(i, True)
    lse_ref[0] = stat_ref[0] + jnp.log(stat_ref[1])
    z = jnp.zeros((rows, wo_ref.shape[-1]), jnp.float32)
    for h in range(heads):
        out = (acc_ref[h] / stat_ref[1, h:h + 1, :]).T
        of_ref[0, :, h * dim:(h + 1) * dim] = out
        o_ref[0, :, h * dim:(h + 1) * dim] = bf(out)
    z = bf(dot(o_ref[0], wo_ref[...]))
    z_ref[0] = z
    zf = z.astype(jnp.float32)
    post = bf(zf * inv_rms(zf) * (1.0 + gain_ref[...]))
    y_ref[0] = bf(x_ref[0].astype(jnp.float32) + post.astype(jnp.float32))


def norm_grad(u, gain, cot):
    r = inv_rms(u)
    g = cot * (1.0 + gain)
    du = r * g - u * (r * r * r) * jnp.mean(g * u, axis=-1, keepdims=True)
    return du, cot * (u * r)


def fold_rows(values, ref):
    part = jnp.sum(values.reshape(values.shape[0] // 8, 8, values.shape[1]), axis=0)

    @pl.when(pl.program_id(0) == 0)
    def _():
        ref[...] = part

    @pl.when(pl.program_id(0) != 0)
    def _():
        ref[...] += part


def mid_kernel(heads, dy_ref, z_ref, of_ref, wo_ref, gain_ref, dz_ref, do_ref, delta_ref, dgain_ref):
    rows = dy_ref.shape[1]
    dim = of_ref.shape[-1] // heads
    dz, dgain = norm_grad(z_ref[0].astype(jnp.float32), gain_ref[...], dy_ref[0].astype(jnp.float32))
    fold_rows(dgain, dgain_ref)
    dz = bf(dz)
    dz_ref[0] = dz
    lane = lax.broadcasted_iota(jnp.int32, (rows, 128), 1)
    cols = jnp.zeros((rows, 128), jnp.float32)
    for h in range(heads):
        sl = slice(h * dim, (h + 1) * dim)
        do = bf(dot(dz, wo_ref[sl, :], NT))
        do_ref[0, :, sl] = do
        cols = jnp.where(lane == h, jnp.sum(do.astype(jnp.float32) * of_ref[0, :, sl], axis=-1, keepdims=True), cols)
    delta_ref[0] = cols.T[:8, :]


def bwd_kernel(heads, q_ref, do_ref, lse_ref, delta_ref, cos_ref, sin_ref, k_ref, kt_ref, v_ref, dq_ref, dk_ref, dv_ref, dqt_ref, dka_ref, dva_ref):
    i = pl.num_programs(0) - 1 - pl.program_id(0)
    dim = k_ref.shape[-1]

    @pl.when(pl.program_id(0) == 0)
    def _():
        dka_ref[...] = jnp.zeros_like(dka_ref)
        dva_ref[...] = jnp.zeros_like(dva_ref)

    dqt_ref[...] = jnp.zeros_like(dqt_ref)

    def block(j, masked):
        key, key_t, val = k_ref[j], kt_ref[j], v_ref[j]
        for h in range(heads):
            qh = q_ref[0, :, h * dim:(h + 1) * dim]
            doh = do_ref[0, :, h * dim:(h + 1) * dim]
            t = jnp.tanh(dot(key, qh, NT) * (1.0 / SOFT_CAP))
            p = jnp.exp(SOFT_CAP * t - lse_ref[0, h:h + 1, :])
            if masked:
                allowed = lax.broadcasted_iota(jnp.int32, t.shape, 0) <= lax.broadcasted_iota(jnp.int32, t.shape, 1)
                p = jnp.where(allowed, p, 0.0)
            dp = dot(val, doh, NT)
            ds = bf(p * (dp - delta_ref[0, h:h + 1, :]) * (1.0 - t * t))
            dva_ref[j] += dot(bf(p), doh)
            dka_ref[j] += dot(ds, qh)
            dqt_ref[h] += dot(key_t, ds)

    def body(j, carry):
        block(j, False)
        return carry

    lax.fori_loop(0, i, body, 0)
    block(i, True)
    cosine, sine = cos_ref[0], sin_ref[0]
    for h in range(heads):
        dq_ref[0, :, h * dim:(h + 1) * dim] = bf(rotate_back(dqt_ref[h].T, cosine, sine) * QUERY_SCALE ** -0.5)
    dk_ref[0] = bf(rotate_back(dka_ref[i], cosine, sine))
    dv_ref[0] = bf(dva_ref[i])


def post_kernel(dq_ref, dk_ref, dv_ref, x_ref, dy_ref, gain_ref, wq_ref, wk_ref, wv_ref, dx_ref, dgain_ref):
    da = dot(dq_ref[0], wq_ref[...], NT) + dot(dk_ref[0], wk_ref[...], NT) + dot(dv_ref[0], wv_ref[...], NT)
    du, dgain = norm_grad(x_ref[0].astype(jnp.float32), gain_ref[...], da)
    fold_rows(dgain, dgain_ref)
    dx_ref[0] = bf(dy_ref[0].astype(jnp.float32) + du)


def piece(*shape, order=None):
    index = (lambda i: (i, 0, 0)) if order is None else (lambda i: (order - 1 - i, 0, 0))
    return pl.BlockSpec((1,) + shape, index)


def whole(*shape):
    zeros = (0,) * len(shape)
    return pl.BlockSpec(shape, lambda i: zeros)


def call(kernel, name, pieces, in_specs, outs, scratch, flops, *args):
    return pl.pallas_call(
        kernel,
        name=name,
        grid=(pieces,),
        in_specs=in_specs,
        out_specs=[spec for spec, _, _ in outs],
        out_shape=[jax.ShapeDtypeStruct(shape, dtype) for _, shape, dtype in outs],
        scratch_shapes=scratch,
        compiler_params=pltpu.CompilerParams(dimension_semantics=("arbitrary",), vmem_limit_bytes=60000 * 1024),
        cost_estimate=pl.CostEstimate(flops=flops, bytes_accessed=8 * 2 ** 20, transcendentals=0),
    )(*args)


MESH = pl.DeviceIdType.MESH


def at(ref, i, n):
    return ref.at[:, pl.ds(pl.multiple_of(i * n, n), n)]


def greet(me, count):
    barrier = pltpu.get_barrier_semaphore()
    for step in range(1, count):
        pl.semaphore_signal(barrier, inc=1, device_id={"cp": lax.rem(me + step, count)}, device_id_type=MESH)
    pl.semaphore_wait(barrier, count - 1)


def near_first(count):
    return [step for pair in zip(range(1, count // 2 + 1), range(count - 1, count // 2 - 1, -1)) for step in pair][:count - 1]


def distance(t, count):
    return jnp.where(lax.rem(t, 2) == 1, (t + 1) // 2, lax.rem(count - t // 2, count))


class Exchange:
    def __init__(self, src, dst, send_sem, recv_sem, me, count):
        self.src, self.dst, self.send_sem, self.recv_sem, self.me, self.count = src, dst, send_sem, recv_sem, me, count

    def copy(self, step):
        to = lax.rem(self.me + step, self.count)
        return pltpu.make_async_remote_copy(
            src_ref=self.src.at[to], dst_ref=self.dst.at[self.me], send_sem=self.send_sem.at[to],
            recv_sem=self.recv_sem.at[self.me], device_id={"cp": to}, device_id_type=MESH)

    def own(self):
        return pltpu.make_async_copy(self.src.at[self.me], self.dst.at[self.me], self.recv_sem.at[self.me])

    def start(self):
        for step in near_first(self.count):
            self.copy(step).start()
        self.own().start()

    def wait_from(self, source):
        pltpu.make_async_copy(self.dst.at[source], self.dst.at[source], self.recv_sem.at[source]).wait()

    def wait_sent(self):
        for step in near_first(self.count):
            self.copy(step).wait_send()


def front_kernel(count, heads, x_in, dy_in, angle, gain_pre, gain_post, wq_in, wk_in, wv_in, wo_in,
                 x_out, dy_out, cos_out, sin_out, actt_out, q_out, k_out, kt_out, v_out, y_out, do_out, dwo_out, lse_out, delta_out, dpost_out,
                 x, dy, wq, wk, wv, wo, cosine, sine, actt, q, k, kt, v, vt, of, ot, z, do, dwo, acc, stat,
                 x_send, x_recv, dy_send, dy_recv, w_sem, out_sem, dwo_sem):
    me = lax.axis_index("cp")
    rows, model = x.shape[1:]
    dim = k.shape[-1]
    width = heads * dim
    greet(me, count)
    x_move = Exchange(x_in, x, x_send, x_recv, me, count)
    dy_move = Exchange(dy_in, dy, dy_send, dy_recv, me, count)
    x_move.start()
    loads = [pltpu.make_async_copy(a, b, w_sem.at[n]) for n, (a, b) in enumerate(((wq_in, wq), (wk_in, wk), (wv_in, wv), (wo_in, wo)))]
    for load in loads:
        load.start()

    def tables(j, carry):
        cosine[j] = jnp.cos(angle[j])
        sine[j] = jnp.sin(angle[j])
        return carry

    lax.fori_loop(0, count, tables, 0)
    for load in loads:
        load.wait()

    def pre(t, carry):
        j = lax.rem(me + count - distance(t, count), count)
        x_move.wait_from(j)

        @pl.when(t == count - 1)
        def _():
            dy_move.start()

        xf = x[j].astype(jnp.float32)
        act = xf * inv_rms(xf) * (1.0 + gain_pre[...])
        at(actt, j, rows)[...] = bf(act.T)
        act = bf(act)
        c, s = cosine[j], sine[j]
        for h in range(heads):
            cols = slice(h * dim, (h + 1) * dim)
            qh = bf(dot(act, wq[:, cols])).astype(jnp.float32)
            q[j, :, cols] = bf(rotate(qh, c, s) * QUERY_SCALE ** -0.5)
        kh = rotate(bf(dot(act, wk[...])).astype(jnp.float32), c, s)
        k[j] = bf(kh)
        kt[j] = bf(kh.T)
        vh = dot(act, wv[...])
        v[j] = bf(vh)
        vt[j] = bf(vh.T)
        return carry

    lax.fori_loop(0, count, pre, 0)
    early = [pltpu.make_async_copy(a, b, out_sem.at[n]) for n, (a, b) in enumerate(
        ((x, x_out), (cosine, cos_out), (sine, sin_out), (actt, actt_out), (q, q_out), (k, k_out), (kt, kt_out), (v, v_out)))]
    for copy in early:
        copy.start()
    early[0].wait()

    def attend(i, carry):
        acc[...] = jnp.zeros_like(acc)
        stat[0] = jnp.full(stat.shape[1:], -1e30, jnp.float32)
        stat[1] = jnp.zeros(stat.shape[1:], jnp.float32)

        def block(j, masked):
            key, val_t = k[j], vt[j]
            for h in range(heads):
                s = dot(key, q[i, :, h * dim:(h + 1) * dim], NT)
                c = SOFT_CAP * jnp.tanh(s * (1.0 / SOFT_CAP))
                if masked:
                    allowed = lax.broadcasted_iota(jnp.int32, s.shape, 0) <= lax.broadcasted_iota(jnp.int32, s.shape, 1)
                    c = jnp.where(allowed, c, -1e30)
                old = stat[0, h:h + 1, :]
                new = jnp.maximum(old, jnp.max(c, axis=0, keepdims=True))
                scale = jnp.exp(old - new)
                p = jnp.exp(c - new)
                stat[1, h:h + 1, :] = stat[1, h:h + 1, :] * scale + jnp.sum(p, axis=0, keepdims=True)
                stat[0, h:h + 1, :] = new
                acc[h] = acc[h] * scale + dot(val_t, bf(p))

        def body(j, carry):
            block(j, False)
            return carry

        lax.fori_loop(0, i, body, 0)
        block(i, True)
        lse_out[i] = stat[0] + jnp.log(stat[1])
        parts = []
        for h in range(heads):
            out_t = acc[h] / stat[1, h:h + 1, :]
            at(ot.at[h * dim:(h + 1) * dim], i, rows)[...] = bf(out_t)
            out = out_t.T
            of[i, :, h * dim:(h + 1) * dim] = out
            parts.append(bf(out))
        zb = bf(dot(jnp.concatenate(parts, axis=1), wo[...]))
        z[pl.ds(pl.multiple_of(i * rows, rows), rows), :] = zb
        zf = zb.astype(jnp.float32)
        post = bf(zf * inv_rms(zf) * (1.0 + gain_post[...]))
        x[i] = bf(x[i].astype(jnp.float32) + post.astype(jnp.float32))
        return carry

    lax.fori_loop(0, count, attend, 0)
    y_copy = pltpu.make_async_copy(x, y_out, out_sem.at[8])
    y_copy.start()
    dpost_out[...] = jnp.zeros_like(dpost_out)

    def mid(t, carry):
        j = lax.rem(me + count - distance(t, count), count)
        dy_move.wait_from(j)
        rws = pl.ds(pl.multiple_of(j * rows, rows), rows)
        dz, dgain = norm_grad(z[rws, :].astype(jnp.float32), gain_post[...], dy[j].astype(jnp.float32))
        dpost_out[...] += jnp.sum(dgain.reshape(rows // 8, 8, model), axis=0)
        dz = bf(dz)
        z[rws, :] = dz
        lane = lax.broadcasted_iota(jnp.int32, (rows, 128), 1)
        cols = jnp.zeros((rows, 128), jnp.float32)
        for h in range(heads):
            sl = slice(h * dim, (h + 1) * dim)
            doh = bf(dot(dz, wo[sl, :], NT))
            do[j, :, sl] = doh
            cols = jnp.where(lane == h, jnp.sum(doh.astype(jnp.float32) * of[j, :, sl], axis=-1, keepdims=True), cols)
        delta_out[j] = cols.T[:8, :]
        return carry

    lax.fori_loop(0, count, mid, 0)
    late = [pltpu.make_async_copy(dy, dy_out, out_sem.at[9]), pltpu.make_async_copy(do, do_out, out_sem.at[10])]
    for copy in late:
        copy.start()

    def put(h, slot):
        return pltpu.make_async_copy(dwo.at[slot], dwo_out.at[h], dwo_sem.at[slot])

    def weight(h, carry):
        slot = lax.rem(h, 2)

        @pl.when(h >= 2)
        def _():
            put(h - 2, slot).wait()

        dwo[slot] = dot(ot[pl.ds(pl.multiple_of(h * dim, dim), dim), :], z[...])
        put(h, slot).start()
        return carry

    lax.fori_loop(0, heads, weight, 0)
    for h in range(heads - 2, heads):
        put(h, h % 2).wait()
    for copy in early[1:] + [y_copy] + late:
        copy.wait()
    x_move.wait_sent()
    dy_move.wait_sent()


def front(count, heads, x_in, dy_in, angle, gain_pre, gain_post, wq, wk, wv, wo):
    bf16, f32 = jnp.bfloat16, jnp.float32
    _, rows, model = x_in.shape
    dim = wk.shape[1]
    width = heads * dim
    tokens = count * rows
    seq = lambda cols, dtype=bf16: ((count, rows, cols), dtype)
    kv = [seq(dim)] * 4
    hbm = pl.BlockSpec(memory_space=pl.ANY)
    vmem = pl.BlockSpec(memory_space=pltpu.VMEM)
    stat = ((count, 8, rows), f32)
    outs = [seq(model), seq(model), seq(dim // 2, f32), seq(dim // 2, f32), ((model, tokens), bf16), seq(width)] + kv[:3] + [
        seq(model), seq(width), ((heads, dim, model), f32), stat, stat, ((8, model), f32)]
    scratch = [seq(model), seq(model), (wq.shape, bf16), (wk.shape, bf16), (wv.shape, bf16), (wo.shape, bf16), seq(dim // 2, f32), seq(dim // 2, f32),
               ((model, tokens), bf16), seq(width)] + kv + [seq(width, f32), ((width, tokens), bf16), ((tokens, model), bf16), seq(width),
               ((2, dim, model), f32), ((heads, dim, rows), f32), ((2, 8, rows), f32)]
    sems = [count, count, count, count, 4, 11, 2]
    return pl.pallas_call(
        functools.partial(front_kernel, count, heads),
        name="front",
        in_specs=[hbm, hbm, vmem, vmem, vmem, hbm, hbm, hbm, hbm],
        out_specs=[hbm] * 12 + [vmem] * 3,
        out_shape=[jax.ShapeDtypeStruct(*o) for o in outs],
        scratch_shapes=[pltpu.VMEM(*s) for s in scratch] + [pltpu.SemaphoreType.DMA((n,)) for n in sems],
        compiler_params=pltpu.CompilerParams(collective_id=1, has_side_effects=True, vmem_limit_bytes=67000000),
        cost_estimate=pl.CostEstimate(flops=10 ** 10, bytes_accessed=8 * 2 ** 20, transcendentals=0),
    )(x_in, dy_in, angle, gain_pre, gain_post, wq, wk, wv, wo)


def exchange(values, count):
    me = lax.axis_index("cp")
    out = jnp.zeros_like(values)
    own = lax.dynamic_slice_in_dim(values, me, 1, 0)
    parts = [(me, own)]
    for step in (4, 3, 5, 2, 6, 7, 1):
        send = lax.dynamic_slice_in_dim(values, lax.rem(me + step, count), 1, 0)
        got = lax.ppermute(send, "cp", [(d, (d + step) % count) for d in range(count)])
        parts.append((lax.rem(me + count - step, count), got))
    for at, part in parts:
        out = lax.dynamic_update_slice_in_dim(out, part, at, 0)
    return out


def solution(mesh):
    count = mesh.shape["cp"]

    def local_step(x_in, positions, dy_out, w_query, w_key, w_value, w_out, w_pre, w_post):
        batch, rows, model = x_in.shape
        heads, dim = w_query.shape[1], w_query.shape[2]
        width = heads * dim
        pieces = count
        bf16, f32 = jnp.bfloat16, jnp.float32
        wq = w_query.reshape(model, width)
        wk = w_key.reshape(model, dim)
        wv = w_value.reshape(model, dim)
        wo = w_out.reshape(width, model)
        gain_pre = w_pre.reshape(1, model)
        gain_post = w_post.reshape(1, model)

        pos = lax.all_to_all(positions, "cp", 0, 0, tiled=True)
        inv_freq = ROPE_BASE ** (jnp.arange(dim // 2, dtype=f32) * (-2.0 / dim))
        angle = pos.astype(f32)[:, :, None] * inv_freq
        x, dy, cosine, sine, actt, q, k, kt, v, y, do, dwo, lse, delta, dpost = front(
            count, heads, x_in, dy_out, angle, gain_pre, gain_post, wq, wk, wv, wo)
        tokens = pieces * rows
        y_out = lax.all_to_all(y, "cp", 0, 0, tiled=True)
        dwo = lax.psum(dwo, "cp")

        dq, dk, dv = call(
            functools.partial(bwd_kernel, heads), "bwd", pieces,
            [piece(rows, width, order=pieces), piece(rows, width, order=pieces), piece(8, rows, order=pieces), piece(8, rows, order=pieces),
             piece(rows, dim // 2, order=pieces), piece(rows, dim // 2, order=pieces),
             whole(pieces, rows, dim), whole(pieces, dim, rows), whole(pieces, rows, dim)],
            [(piece(rows, width, order=pieces), (pieces, rows, width), bf16),
             (piece(rows, dim, order=pieces), (pieces, rows, dim), bf16), (piece(rows, dim, order=pieces), (pieces, rows, dim), bf16)],
            [pltpu.VMEM((heads, dim, rows), f32), pltpu.VMEM((pieces, rows, dim), f32), pltpu.VMEM((pieces, rows, dim), f32)], 12 * 10 ** 9,
            q, do, lse, delta, cosine, sine, k, kt, v)

        dwq = dot(actt, dq.reshape(tokens, width))
        dwk = dot(actt, dk.reshape(tokens, dim))
        dwv = dot(actt, dv.reshape(tokens, dim))
        dx, dpre = call(
            post_kernel, "post", pieces,
            [piece(rows, width), piece(rows, dim), piece(rows, dim), piece(rows, model), piece(rows, model), whole(1, model),
             whole(model, width), whole(model, dim), whole(model, dim)],
            [(piece(rows, model), (pieces, rows, model), bf16), (whole(8, model), (8, model), f32)],
            [], 2 * 10 ** 9, dq, dk, dv, x, dy, gain_pre, wq, wk, wv)
        dwq, dwk, dwv, dpre, dpost = lax.psum((dwq, dwk, dwv, jnp.sum(dpre, axis=0), jnp.sum(dpost, axis=0)), "cp")
        dx_in = lax.all_to_all(dx, "cp", 0, 0, tiled=True)
        return (y_out, dx_in, dwq.reshape(model, heads, dim), dwk.reshape(model, 1, dim), dwv.reshape(model, 1, dim),
                dwo.reshape(heads, dim, model), dpre, dpost)

    seq_spec = P("dp", "cp", None)
    in_specs = (seq_spec, P("dp", "cp"), seq_spec, P(), P(), P(), P(), P(), P())
    out_specs = (seq_spec, seq_spec, P("dp", None, None), P("dp", None, None), P("dp", None, None), P("dp", None, None), P("dp"), P("dp"))
    return jax.shard_map(local_step, mesh=mesh, in_specs=in_specs, out_specs=out_specs, check_vma=False)
```

```python
import functools

import jax
import jax.numpy as jnp
from jax import lax
from jax.experimental import pallas as pl
from jax.experimental.pallas import tpu as pltpu
from jax.sharding import PartitionSpec as P

NORM_EPS = 1e-6
SOFT_CAP = 50.0
QUERY_SCALE = 144.0
ROPE_BASE = 10000.0

NN = (((1,), (0,)), ((), ()))
NT = (((1,), (1,)), ((), ()))
TN = (((0,), (0,)), ((), ()))

def dot(a, b, dims=NN):
    return lax.dot_general(a, b, dims, preferred_element_type=jnp.float32)


def rope_tables(positions, head_dim):
    half = head_dim // 2
    inv_freq = ROPE_BASE ** (jnp.arange(half, dtype=jnp.float32) * (-2.0 / head_dim))
    angles = positions.astype(jnp.float32)[:, :, None] * inv_freq
    return jnp.cos(angles), jnp.sin(angles)


def rotate(values, cosine, sine):
    half = values.shape[-1] // 2
    first = values[..., :half]
    second = values[..., half:]
    return jnp.concatenate([first * cosine - second * sine, second * cosine + first * sine], axis=-1)


def rotate_back(values, cosine, sine):
    half = values.shape[-1] // 2
    first = values[..., :half]
    second = values[..., half:]
    return jnp.concatenate([first * cosine + second * sine, second * cosine - first * sine], axis=-1)


def bf(values):
    return values.astype(jnp.bfloat16)


def inv_rms(values):
    return lax.rsqrt(jnp.mean(values * values, axis=-1, keepdims=True) + NORM_EPS)


def norm_grad(u, gain, cot):
    r = inv_rms(u)
    g = cot * (1.0 + gain)
    du = r * g - u * (r * r * r) * jnp.mean(g * u, axis=-1, keepdims=True)
    return du, cot * (u * r)


MESH = pl.DeviceIdType.MESH


def at(ref, i, n):
    return ref.at[:, pl.ds(pl.multiple_of(i * n, n), n)]


def greet(me, count):
    barrier = pltpu.get_barrier_semaphore()
    for step in range(1, count):
        pl.semaphore_signal(barrier, inc=1, device_id={"cp": lax.rem(me + step, count)}, device_id_type=MESH)
    pl.semaphore_wait(barrier, count - 1)


def near_first(count):
    return [step for pair in zip(range(1, count // 2 + 1), range(count - 1, count // 2 - 1, -1)) for step in pair][:count - 1]


def distance(t, count):
    return jnp.where(lax.rem(t, 2) == 1, (t + 1) // 2, lax.rem(count - t // 2, count))


class Exchange:
    def __init__(self, src, dst, send_sem, recv_sem, me, count):
        self.src, self.dst, self.send_sem, self.recv_sem, self.me, self.count = src, dst, send_sem, recv_sem, me, count

    def copy(self, step):
        to = lax.rem(self.me + step, self.count)
        return pltpu.make_async_remote_copy(
            src_ref=self.src.at[to], dst_ref=self.dst.at[self.me], send_sem=self.send_sem.at[to],
            recv_sem=self.recv_sem.at[self.me], device_id={"cp": to}, device_id_type=MESH)

    def own(self):
        return pltpu.make_async_copy(self.src.at[self.me], self.dst.at[self.me], self.recv_sem.at[self.me])

    def start(self, steps):
        for step in steps:
            if step:
                self.copy(step).start()
            else:
                self.own().start()

    def wait_from(self, source):
        pltpu.make_async_copy(self.dst.at[source], self.dst.at[source], self.recv_sem.at[source]).wait()

    def wait_sent(self):
        for step in near_first(self.count):
            self.copy(step).wait_send()


def front_kernel(count, heads, x_in, dy_in, angle, gain_pre, gain_post, wq_in, wk_in, wv_in, wo_in,
                 x_out, dy_out, cos_out, sin_out, actt_out, q_out, k_out, kt_out, v_out, y_out, do_out, dwo_out, lse_out, delta_out, dpost_out,
                 x, dy, wq, wk, wv, wo, cosine, sine, actt, q, k, kt, v, vt, of, ot, z, do, dwo, acc, stat,
                 x_send, x_recv, dy_send, dy_recv, w_sem, out_sem, dwo_sem):
    me = lax.axis_index("cp")
    rows, model = x.shape[1:]
    dim = k.shape[-1]
    width = heads * dim
    greet(me, count)
    x_move = Exchange(x_in, x, x_send, x_recv, me, count)
    dy_move = Exchange(dy_in, dy, dy_send, dy_recv, me, count)
    x_move.start(near_first(count) + [0])
    loads = [pltpu.make_async_copy(a, b, w_sem.at[n]) for n, (a, b) in enumerate(((wq_in, wq), (wk_in, wk), (wv_in, wv), (wo_in, wo)))]
    for load in loads:
        load.start()

    def tables(j, carry):
        cosine[j] = jnp.cos(angle[j])
        sine[j] = jnp.sin(angle[j])
        return carry

    lax.fori_loop(0, count, tables, 0)
    for load in loads:
        load.wait()

    def pre(t, carry):
        j = lax.rem(me + count - distance(t, count), count)
        x_move.wait_from(j)

        @pl.when(t == count - 1)
        def _():
            dy_move.start(near_first(count) + [0])

        xf = x[j].astype(jnp.float32)
        act = xf * inv_rms(xf) * (1.0 + gain_pre[...])
        at(actt, j, rows)[...] = bf(act.T)
        act = bf(act)
        c, s = cosine[j], sine[j]
        for h in range(heads):
            cols = slice(h * dim, (h + 1) * dim)
            qh = bf(dot(act, wq[:, cols])).astype(jnp.float32)
            q[j, :, cols] = bf(rotate(qh, c, s) * QUERY_SCALE ** -0.5)
        kh = rotate(bf(dot(act, wk[...])).astype(jnp.float32), c, s)
        k[j] = bf(kh)
        kt[j] = bf(kh.T)
        vh = dot(act, wv[...])
        v[j] = bf(vh)
        vt[j] = bf(vh.T)
        return carry

    lax.fori_loop(0, count, pre, 0)
    early = [pltpu.make_async_copy(a, b, out_sem.at[n]) for n, (a, b) in enumerate(
        ((x, x_out), (cosine, cos_out), (sine, sin_out), (actt, actt_out), (q, q_out), (k, k_out), (kt, kt_out), (v, v_out)))]
    for copy in early:
        copy.start()
    early[0].wait()

    def attend(i, carry):
        acc[...] = jnp.zeros_like(acc)
        stat[0] = jnp.full(stat.shape[1:], -1e30, jnp.float32)
        stat[1] = jnp.zeros(stat.shape[1:], jnp.float32)

        def block(j, masked):
            key, val_t = k[j], vt[j]
            for h in range(heads):
                s = dot(key, q[i, :, h * dim:(h + 1) * dim], NT)
                c = SOFT_CAP * jnp.tanh(s * (1.0 / SOFT_CAP))
                if masked:
                    allowed = lax.broadcasted_iota(jnp.int32, s.shape, 0) <= lax.broadcasted_iota(jnp.int32, s.shape, 1)
                    c = jnp.where(allowed, c, -1e30)
                old = stat[0, h:h + 1, :]
                new = jnp.maximum(old, jnp.max(c, axis=0, keepdims=True))
                scale = jnp.exp(old - new)
                p = jnp.exp(c - new)
                stat[1, h:h + 1, :] = stat[1, h:h + 1, :] * scale + jnp.sum(p, axis=0, keepdims=True)
                stat[0, h:h + 1, :] = new
                acc[h] = acc[h] * scale + dot(val_t, bf(p))

        def body(j, carry):
            block(j, False)
            return carry

        lax.fori_loop(0, i, body, 0)
        block(i, True)
        lse_out[i] = stat[0] + jnp.log(stat[1])
        parts = []
        for h in range(heads):
            out_t = acc[h] / stat[1, h:h + 1, :]
            at(ot.at[h * dim:(h + 1) * dim], i, rows)[...] = bf(out_t)
            out = out_t.T
            of[i, :, h * dim:(h + 1) * dim] = out
            parts.append(bf(out))
        zb = bf(dot(jnp.concatenate(parts, axis=1), wo[...]))
        z[pl.ds(pl.multiple_of(i * rows, rows), rows), :] = zb
        zf = zb.astype(jnp.float32)
        post = bf(zf * inv_rms(zf) * (1.0 + gain_post[...]))
        x[i] = bf(x[i].astype(jnp.float32) + post.astype(jnp.float32))
        return carry

    lax.fori_loop(0, count, attend, 0)
    y_copy = pltpu.make_async_copy(x, y_out, out_sem.at[8])
    y_copy.start()
    dpost_out[...] = jnp.zeros_like(dpost_out)

    def mid(t, carry):
        j = lax.rem(me + count - distance(t, count), count)
        dy_move.wait_from(j)
        rws = pl.ds(pl.multiple_of(j * rows, rows), rows)
        dz, dgain = norm_grad(z[rws, :].astype(jnp.float32), gain_post[...], dy[j].astype(jnp.float32))
        dpost_out[...] += jnp.sum(dgain.reshape(rows // 8, 8, model), axis=0)
        dz = bf(dz)
        z[rws, :] = dz
        lane = lax.broadcasted_iota(jnp.int32, (rows, 128), 1)
        cols = jnp.zeros((rows, 128), jnp.float32)
        for h in range(heads):
            sl = slice(h * dim, (h + 1) * dim)
            doh = bf(dot(dz, wo[sl, :], NT))
            do[j, :, sl] = doh
            cols = jnp.where(lane == h, jnp.sum(doh.astype(jnp.float32) * of[j, :, sl], axis=-1, keepdims=True), cols)
        delta_out[j] = cols.T[:8, :]
        return carry

    lax.fori_loop(0, count, mid, 0)
    late = [pltpu.make_async_copy(dy, dy_out, out_sem.at[9]), pltpu.make_async_copy(do, do_out, out_sem.at[10])]
    for copy in late:
        copy.start()

    def put(h, slot):
        return pltpu.make_async_copy(dwo.at[slot], dwo_out.at[h], dwo_sem.at[slot])

    def weight(h, carry):
        slot = lax.rem(h, 2)

        @pl.when(h >= 2)
        def _():
            put(h - 2, slot).wait()

        dwo[slot] = dot(ot[pl.ds(pl.multiple_of(h * dim, dim), dim), :], z[...])
        put(h, slot).start()
        return carry

    lax.fori_loop(0, heads, weight, 0)
    for h in range(heads - 2, heads):
        put(h, h % 2).wait()
    for copy in early[1:] + [y_copy] + late:
        copy.wait()
    x_move.wait_sent()
    dy_move.wait_sent()


def front(count, heads, x_in, dy_in, angle, gain_pre, gain_post, wq, wk, wv, wo):
    bf16, f32 = jnp.bfloat16, jnp.float32
    _, rows, model = x_in.shape
    dim = wk.shape[1]
    width = heads * dim
    tokens = count * rows
    seq = lambda cols, dtype=bf16: ((count, rows, cols), dtype)
    kv = [seq(dim)] * 4
    hbm = pl.BlockSpec(memory_space=pl.ANY)
    vmem = pl.BlockSpec(memory_space=pltpu.VMEM)
    stat = ((count, 8, rows), f32)
    outs = [seq(model), seq(model), seq(dim // 2, f32), seq(dim // 2, f32), ((model, tokens), bf16), seq(width)] + kv[:3] + [
        seq(model), seq(width), ((heads, dim, model), f32), stat, stat, ((8, model), f32)]
    scratch = [seq(model), seq(model), (wq.shape, bf16), (wk.shape, bf16), (wv.shape, bf16), (wo.shape, bf16), seq(dim // 2, f32), seq(dim // 2, f32),
               ((model, tokens), bf16), seq(width)] + kv + [seq(width, f32), ((width, tokens), bf16), ((tokens, model), bf16), seq(width),
               ((2, dim, model), f32), ((heads, dim, rows), f32), ((2, 8, rows), f32)]
    sems = [count, count, count, count, 4, 11, 2]
    return pl.pallas_call(
        functools.partial(front_kernel, count, heads),
        name="front",
        in_specs=[hbm, hbm, vmem, vmem, vmem, hbm, hbm, hbm, hbm],
        out_specs=[hbm] * 12 + [vmem] * 3,
        out_shape=[jax.ShapeDtypeStruct(*o) for o in outs],
        scratch_shapes=[pltpu.VMEM(*s) for s in scratch] + [pltpu.SemaphoreType.DMA((n,)) for n in sems],
        compiler_params=pltpu.CompilerParams(collective_id=1, has_side_effects=True, vmem_limit_bytes=67000000),
        cost_estimate=pl.CostEstimate(flops=10 ** 10, bytes_accessed=8 * 2 ** 20, transcendentals=0),
    )(x_in, dy_in, angle, gain_pre, gain_post, wq, wk, wv, wo)


class SumAll:
    def __init__(self, total, out, slots, send, recv, keep, me):
        self.total, self.out, self.send, self.recv, self.keep = total, out, send, recv, keep
        self.from_core, self.from_first, self.from_second = slots
        core, chip = lax.rem(me, 2), me // 2
        self.core = core
        swap = chip + 1 - 2 * lax.rem(chip, 2)
        turn = lax.rem(chip + 3 + 2 * lax.rem(chip, 2), 4)
        low, high = lax.rem((chip + 1) // 2, 2), chip // 2
        self.sibling = me + 1 - 2 * core
        self.first = (swap * 2 + core, turn * 2 + core)
        self.second = (turn * 2 + core, swap * 2 + core)
        self.sub = (low, high)
        self.quarter = (high, low)
        self.base = (core * 8, core * 8 + 4)

    def move(self, start, blocks, target, at_block, sem, device, source=None):
        source = self.total if source is None else source
        return pltpu.make_async_remote_copy(
            src_ref=source.at[pl.ds(start, blocks)], dst_ref=target.at[pl.ds(at_block, blocks)], send_sem=self.send.at[sem],
            recv_sem=self.recv.at[sem], device_id={"cp": device}, device_id_type=MESH)

    def half(self):
        return self.move((1 - self.core) * 8, 8, self.from_core, 0, 0, self.sibling)

    def reduce_first(self, s):
        return self.move(self.base[s] + (1 - self.sub[s]) * 2, 2, self.from_first, 2 * s, 1 + s, self.first[s])

    def reduce_second(self, s):
        return self.move(self.base[s] + self.sub[s] * 2 + 1 - self.quarter[s], 1, self.from_second, s, 3 + s, self.second[s])

    def gather_second(self, s):
        at_block = self.base[s] + self.sub[s] * 2 + self.quarter[s]
        return self.move(at_block, 1, self.out, at_block, 5 + s, self.second[s])

    def keep_own(self, s):
        block = pl.ds(self.base[s] + self.sub[s] * 2 + self.quarter[s], 1)
        return pltpu.make_async_copy(self.total.at[block], self.out.at[block], self.keep.at[s])

    def gather_first(self, s):
        at_block = self.base[s] + self.sub[s] * 2
        return self.move(at_block, 2, self.out, at_block, 7 + s, self.first[s], self.out)

    def share_own(self, s):
        at_block = self.base[s] + self.sub[s] * 2
        return self.move(at_block, 2, self.out, at_block, 9 + s, self.sibling, self.out)

    def share_other(self, s):
        at_block = self.base[s] + (1 - self.sub[s]) * 2
        return self.move(at_block, 2, self.out, at_block, 11 + s, self.sibling, self.out)

    def add(self, start, source, at_block, blocks):
        def body(n, carry):
            self.total[start + n] = self.total[start + n] + source[at_block + n]
            return carry

        lax.fori_loop(0, blocks, body, 0)

    def begin(self):
        self.half().start()

    def finish_half(self):
        self.half().wait_recv()
        for s in range(2):
            self.add(self.base[s] + (1 - self.sub[s]) * 2, self.from_core, s * 4 + (1 - self.sub[s]) * 2, 2)
        for s in range(2):
            self.reduce_first(s).start()
        for s in range(2):
            self.add(self.base[s] + self.sub[s] * 2, self.from_core, s * 4 + self.sub[s] * 2, 2)

    def finish_first(self):
        for s in range(2):
            self.reduce_first(s).wait_recv()
            self.add(self.base[s] + self.sub[s] * 2, self.from_first, 2 * s, 2)
            self.reduce_second(s).start()

    def finish_second(self):
        for s in range(2):
            self.reduce_second(s).wait_recv()
            self.add(self.base[s] + self.sub[s] * 2 + self.quarter[s], self.from_second, s, 1)
            self.gather_second(s).start()
            self.keep_own(s).start()

    def finish_gather(self):
        for s in range(2):
            self.gather_second(s).wait_recv()
            self.keep_own(s).wait()
            self.gather_first(s).start()
            self.share_own(s).start()

    def finish_share(self):
        for s in range(2):
            self.gather_first(s).wait_recv()
            self.share_other(s).start()

    def end(self):
        for s in range(2):
            self.share_own(s).wait_recv()
            self.share_other(s).wait_recv()
        self.half().wait_send()
        for s in range(2):
            for step in (self.reduce_first, self.reduce_second, self.gather_second, self.gather_first, self.share_own, self.share_other):
                step(s).wait_send()


def back_kernel(count, heads, y_in, x_in, dy_in, q_in, do_in, k_in, kt_in, v_in, actt_in, cos_in, sin_in, dwo_in, wq_in, wk_in, wv_in,
                lse, delta, dpost, gain_pre,
                y_out, dx_out, dwo_out, dqkv_out, gains_out,
                x, dy, q, do, k, kt, v, actt, cosine, sine, wqkv, dqkv, dqt, dka, dva, dx, dpre, gains,
                wo_sum, wo_half, wo_first, wo_second, qkv_sum, qkv_half, qkv_first, qkv_second,
                y_send, y_recv, dx_send, dx_recv, gain_send, gain_recv, wo_send, wo_recv, qkv_send, qkv_recv, load_sem, piece_sem, wo_keep, qkv_keep):
    me = lax.axis_index("cp")
    rows, model = x.shape[1:]
    dim = k.shape[-1]
    width = heads * dim
    greet(me, count)
    wo_total = SumAll(wo_sum, dwo_out, (wo_half, wo_first, wo_second), wo_send, wo_recv, wo_keep, me)
    qkv_total = SumAll(qkv_sum, dqkv_out, (qkv_half, qkv_first, qkv_second), qkv_send, qkv_recv, qkv_keep, me)
    y_move = Exchange(y_in, y_out, y_send, y_recv, me, count)
    dx_move = Exchange(dx, dx_out, dx_send, dx_recv, me, count)
    order = [0] + near_first(count)

    def fetch(i, slot):
        return [pltpu.make_async_copy(a.at[i], b.at[slot], piece_sem.at[slot, n]) for n, (a, b) in enumerate(
            ((q_in, q), (do_in, do), (x_in, x), (dy_in, dy)))]

    loads = [pltpu.make_async_copy(a, b, load_sem.at[n]) for n, (a, b) in enumerate((
        (dwo_in, wo_sum), (k_in, k), (kt_in, kt), (v_in, v), (cos_in, cosine), (sin_in, sine),
        (wq_in, wqkv.at[:, 0:width]), (wk_in, wqkv.at[:, width:width + dim]), (wv_in, wqkv.at[:, width + dim:]), (actt_in, actt)))]
    for load in loads:
        load.start()
    for load in fetch(count - 1, 0):
        load.start()
    loads[0].wait()
    wo_total.begin()
    dka[...] = jnp.zeros_like(dka)
    dva[...] = jnp.zeros_like(dva)
    dpre[...] = jnp.zeros_like(dpre)
    for load in loads[1:]:
        load.wait()
    wo_total.finish_half()
    y_move.start(order[:4])

    def step(g, carry):
        i = count - 1 - g
        slot = lax.rem(g, 2)

        @pl.when(g < count - 1)
        def _():
            for load in fetch(i - 1, 1 - slot):
                load.start()

        for load in fetch(i, slot):
            load.wait()
        dqt[...] = jnp.zeros_like(dqt)

        def block(j, masked):
            key, key_t, val = k[j], kt[j], v[j]
            for h in range(heads):
                qh = q[slot, :, h * dim:(h + 1) * dim]
                doh = do[slot, :, h * dim:(h + 1) * dim]
                t = jnp.tanh(dot(key, qh, NT) * (1.0 / SOFT_CAP))
                p = jnp.exp(SOFT_CAP * t - lse[i, h:h + 1, :])
                if masked:
                    allowed = lax.broadcasted_iota(jnp.int32, t.shape, 0) <= lax.broadcasted_iota(jnp.int32, t.shape, 1)
                    p = jnp.where(allowed, p, 0.0)
                dp = dot(val, doh, NT)
                ds = bf(p * (dp - delta[i, h:h + 1, :]) * (1.0 - t * t))
                dva[j] += dot(bf(p), doh)
                dka[j] += dot(ds, qh)
                dqt[h] += dot(key_t, ds)

        def body(j, carry):
            block(j, False)
            return carry

        lax.fori_loop(0, i, body, 0)
        block(i, True)
        c, s = cosine[i], sine[i]
        rws = pl.ds(pl.multiple_of(i * rows, rows), rows)
        for h in range(heads):
            dqkv[rws, h * dim:(h + 1) * dim] = bf(rotate_back(dqt[h].T, c, s) * QUERY_SCALE ** -0.5)
        dqkv[rws, width:width + dim] = bf(rotate_back(dka[i], c, s))
        dqkv[rws, width + dim:] = bf(dva[i])
        da = dot(dqkv[rws, :], wqkv[...], NT)
        du, dgain = norm_grad(x[slot].astype(jnp.float32), gain_pre[...], da)
        dpre[...] += jnp.sum(dgain.reshape(rows // 8, 8, model), axis=0)
        dx[i] = bf(dy[slot].astype(jnp.float32) + du)

        @pl.when(g == 1)
        def _():
            wo_total.finish_first()
            y_move.start(order[4:6])

        @pl.when(g == 3)
        def _():
            wo_total.finish_second()
            y_move.start(order[6:])

        @pl.when(g == 5)
        def _():
            wo_total.finish_gather()

        return carry

    lax.fori_loop(0, count, step, 0)
    dx_move.start(order[-3:])
    part = qkv_sum.shape[1] * 4

    def weight(n, carry):
        at_block = lax.rem((1 - qkv_total.core) * 2 + n, 4)
        lhs = actt[pl.ds(pl.multiple_of(at_block * part, 16), part), :]
        qkv_sum[pl.ds(at_block * 4, 4)] = dot(lhs, dqkv[...]).reshape(4, part // 4, width + 2 * dim)

        @pl.when(n == 1)
        def _():
            qkv_total.begin()
            wo_total.finish_share()

        return carry

    lax.fori_loop(0, 4, weight, 0)
    gains[me] = jnp.concatenate([jnp.sum(dpre[...], axis=0, keepdims=True), jnp.sum(dpost[...], axis=0, keepdims=True), jnp.zeros((6, model), jnp.float32)], axis=0)
    qkv_total.finish_half()
    dx_move.start(order[:2])

    def send_gains(step):
        to = lax.rem(me + step, count)
        return pltpu.make_async_remote_copy(
            src_ref=gains.at[me], dst_ref=gains.at[me], send_sem=gain_send.at[to], recv_sem=gain_recv.at[me], device_id={"cp": to}, device_id_type=MESH)

    for n in range(1, count):
        send_gains(n).start()
    qkv_total.finish_first()
    dx_move.start(order[2:4])
    wo_total.end()
    for n in range(1, count):
        source = lax.rem(me + n, count)
        pltpu.make_async_copy(gains.at[source], gains.at[source], gain_recv.at[source]).wait()
    gains_out[...] = jnp.sum(gains[...], axis=0)
    qkv_total.finish_second()
    dx_move.start(order[4:-3])
    qkv_total.finish_gather()
    qkv_total.finish_share()
    qkv_total.end()
    for n in range(1, count):
        send_gains(n).wait_send()
    for source in range(count):
        dx_move.wait_from(source)
    dx_move.wait_sent()
    for source in range(count):
        y_move.wait_from(source)
    y_move.wait_sent()


def back(count, heads, y, x, dy, q, do, k, kt, v, actt, cosine, sine, dwo, wq, wk, wv, lse, delta, dpost, gain_pre):
    bf16, f32 = jnp.bfloat16, jnp.float32
    _, rows, model = x.shape
    dim = wk.shape[1]
    width = heads * dim
    wide = width + 2 * dim
    tokens = count * rows
    seq = lambda cols, dtype=bf16, n=count: ((n, rows, cols), dtype)
    blocks = lambda n, height, cols: ((n, height // 16, cols), f32)
    hbm = pl.BlockSpec(memory_space=pl.ANY)
    vmem = pl.BlockSpec(memory_space=pltpu.VMEM)
    outs = [seq(model), seq(model), blocks(16, width, model), blocks(16, model, wide), ((8, model), f32)]
    scratch = [seq(model, n=2), seq(model, n=2), seq(width, n=2), seq(width, n=2), seq(dim), seq(dim), seq(dim), (actt.shape, bf16),
               seq(dim // 2, f32), seq(dim // 2, f32), ((model, wide), bf16), ((tokens, wide), bf16), ((heads, dim, rows), f32),
               seq(dim, f32), seq(dim, f32), seq(model), ((8, model), f32), ((count, 8, model), f32)]
    scratch += [blocks(n, width, model) for n in (16, 8, 4, 2)] + [blocks(n, model, wide) for n in (16, 8, 4, 2)]
    sems = [(count,)] * 6 + [(13,)] * 4 + [(10,), (2, 4), (2,), (2,)]
    return pl.pallas_call(
        functools.partial(back_kernel, count, heads),
        name="back",
        in_specs=[hbm] * 15 + [vmem] * 4,
        out_specs=[hbm] * 4 + [vmem],
        out_shape=[jax.ShapeDtypeStruct(*o) for o in outs],
        scratch_shapes=[pltpu.VMEM(*s) for s in scratch] + [pltpu.SemaphoreType.DMA(n) for n in sems],
        compiler_params=pltpu.CompilerParams(collective_id=2, has_side_effects=True, vmem_limit_bytes=67000000),
        cost_estimate=pl.CostEstimate(flops=10 ** 10, bytes_accessed=8 * 2 ** 20, transcendentals=0),
    )(y, x, dy, q, do, k, kt, v, actt, cosine, sine, dwo.reshape(16, width // 16, model), wq, wk, wv, lse, delta, dpost, gain_pre)


def solution(mesh):
    count = mesh.shape["cp"]

    def local_step(x_in, positions, dy_out, w_query, w_key, w_value, w_out, w_pre, w_post):
        model = x_in.shape[-1]
        heads, dim = w_query.shape[1], w_query.shape[2]
        width = heads * dim
        f32 = jnp.float32
        wq = w_query.reshape(model, width)
        wk = w_key.reshape(model, dim)
        wv = w_value.reshape(model, dim)
        wo = w_out.reshape(width, model)
        gain_pre = w_pre.reshape(1, model)
        gain_post = w_post.reshape(1, model)

        pos = lax.all_to_all(positions, "cp", 0, 0, tiled=True)
        inv_freq = ROPE_BASE ** (jnp.arange(dim // 2, dtype=f32) * (-2.0 / dim))
        angle = pos.astype(f32)[:, :, None] * inv_freq
        x, dy, cosine, sine, actt, q, k, kt, v, y, do, dwo, lse, delta, dpost = front(
            count, heads, x_in, dy_out, angle, gain_pre, gain_post, wq, wk, wv, wo)
        y_out, dx_in, dwo, dqkv, gains = back(
            count, heads, y, x, dy, q, do, k, kt, v, actt, cosine, sine, dwo, wq, wk, wv, lse, delta, dpost, gain_pre)
        width = heads * dim
        dqkv = dqkv.reshape(model, width + 2 * dim)
        return (y_out, dx_in, dqkv[:, :width].reshape(model, heads, dim), dqkv[:, None, width:width + dim], dqkv[:, None, width + dim:],
                dwo.reshape(heads, dim, model), gains[0], gains[1])

    seq_spec = P("dp", "cp", None)
    in_specs = (seq_spec, P("dp", "cp"), seq_spec, P(), P(), P(), P(), P(), P())
    out_specs = (seq_spec, seq_spec, P("dp", None, None), P("dp", None, None), P("dp", None, None), P("dp", None, None), P("dp"), P("dp"))
    return jax.shard_map(local_step, mesh=mesh, in_specs=in_specs, out_specs=out_specs, check_vma=False)
```

```python
import functools

import jax
import jax.numpy as jnp
from jax import lax
from jax.experimental import pallas as pl
from jax.experimental.pallas import tpu as pltpu
from jax.sharding import PartitionSpec as P

NORM_EPS = 1e-6
SOFT_CAP = 50.0
QUERY_SCALE = 144.0
ROPE_BASE = 10000.0

NN = (((1,), (0,)), ((), ()))
NT = (((1,), (1,)), ((), ()))
TN = (((0,), (0,)), ((), ()))

def dot(a, b, dims=NN):
    return lax.dot_general(a, b, dims, preferred_element_type=jnp.float32)


def rope_tables(positions, head_dim):
    half = head_dim // 2
    inv_freq = ROPE_BASE ** (jnp.arange(half, dtype=jnp.float32) * (-2.0 / head_dim))
    angles = positions.astype(jnp.float32)[:, :, None] * inv_freq
    return jnp.cos(angles), jnp.sin(angles)


def rotate(values, cosine, sine):
    half = values.shape[-1] // 2
    first = values[..., :half]
    second = values[..., half:]
    return jnp.concatenate([first * cosine - second * sine, second * cosine + first * sine], axis=-1)


def rotate_back(values, cosine, sine):
    half = values.shape[-1] // 2
    first = values[..., :half]
    second = values[..., half:]
    return jnp.concatenate([first * cosine + second * sine, second * cosine - first * sine], axis=-1)


def bf(values):
    return values.astype(jnp.bfloat16)


def inv_rms(values):
    return lax.rsqrt(jnp.mean(values * values, axis=-1, keepdims=True) + NORM_EPS)


def norm_grad(u, gain, cot):
    r = inv_rms(u)
    g = cot * (1.0 + gain)
    du = r * g - u * (r * r * r) * jnp.mean(g * u, axis=-1, keepdims=True)
    return du, cot * (u * r)


MESH = pl.DeviceIdType.MESH


def at(ref, i, n):
    return ref.at[:, pl.ds(pl.multiple_of(i * n, n), n)]


def greet(me, count):
    barrier = pltpu.get_barrier_semaphore()
    for step in range(1, count):
        pl.semaphore_signal(barrier, inc=1, device_id={"cp": lax.rem(me + step, count)}, device_id_type=MESH)
    pl.semaphore_wait(barrier, count - 1)


def near_first(count):
    return [step for pair in zip(range(1, count // 2 + 1), range(count - 1, count // 2 - 1, -1)) for step in pair][:count - 1]


def distance(t, count):
    return jnp.where(lax.rem(t, 2) == 1, (t + 1) // 2, lax.rem(count - t // 2, count))


class Exchange:
    def __init__(self, src, dst, send_sem, recv_sem, me, count):
        self.src, self.dst, self.send_sem, self.recv_sem, self.me, self.count = src, dst, send_sem, recv_sem, me, count

    def copy(self, step):
        to = lax.rem(self.me + step, self.count)
        return pltpu.make_async_remote_copy(
            src_ref=self.src.at[to], dst_ref=self.dst.at[self.me], send_sem=self.send_sem.at[to],
            recv_sem=self.recv_sem.at[self.me], device_id={"cp": to}, device_id_type=MESH)

    def own(self):
        return pltpu.make_async_copy(self.src.at[self.me], self.dst.at[self.me], self.recv_sem.at[self.me])

    def start(self, steps):
        for step in steps:
            if step:
                self.copy(step).start()
            else:
                self.own().start()

    def wait_from(self, source):
        pltpu.make_async_copy(self.dst.at[source], self.dst.at[source], self.recv_sem.at[source]).wait()

    def wait_sent(self):
        for step in near_first(self.count):
            self.copy(step).wait_send()


def front_kernel(count, heads, x_in, dy_in, angle, gain_pre, gain_post, wq_in, wk_in, wv_in, wo_in,
                 x_out, dy_out, cos_out, sin_out, actt_out, q_out, k_out, kt_out, v_out, y_out, do_out, dwo_out, lse_out, delta_out, dpost_out,
                 x, dy, wq, wk, wv, wo, cosine, sine, actt, q, k, kt, v, vt, of, ot, z, do, dwo, acc, stat,
                 x_send, x_recv, dy_send, dy_recv, w_sem, out_sem, dwo_sem):
    me = lax.axis_index("cp")
    rows, model = x.shape[1:]
    dim = k.shape[-1]
    width = heads * dim
    greet(me, count)
    x_move = Exchange(x_in, x, x_send, x_recv, me, count)
    dy_move = Exchange(dy_in, dy, dy_send, dy_recv, me, count)
    x_move.start(near_first(count) + [0])
    loads = [pltpu.make_async_copy(a, b, w_sem.at[n]) for n, (a, b) in enumerate(((wq_in, wq), (wk_in, wk), (wv_in, wv), (wo_in, wo)))]
    for load in loads:
        load.start()

    def tables(j, carry):
        cosine[j] = jnp.cos(angle[j])
        sine[j] = jnp.sin(angle[j])
        return carry

    lax.fori_loop(0, count, tables, 0)
    for load in loads:
        load.wait()

    def pre(t, carry):
        j = lax.rem(me + count - distance(t, count), count)
        x_move.wait_from(j)

        @pl.when(t == count - 1)
        def _():
            dy_move.start(near_first(count) + [0])

        xf = x[j].astype(jnp.float32)
        act = xf * inv_rms(xf) * (1.0 + gain_pre[...])
        at(actt, j, rows)[...] = bf(act.T)
        act = bf(act)
        c, s = cosine[j], sine[j]
        for h in range(heads):
            cols = slice(h * dim, (h + 1) * dim)
            qh = bf(dot(act, wq[:, cols])).astype(jnp.float32)
            q[j, :, cols] = bf(rotate(qh, c, s) * QUERY_SCALE ** -0.5)
        kh = rotate(bf(dot(act, wk[...])).astype(jnp.float32), c, s)
        k[j] = bf(kh)
        kt[j] = bf(kh.T)
        vh = dot(act, wv[...])
        v[j] = bf(vh)
        vt[j] = bf(vh.T)
        return carry

    lax.fori_loop(0, count, pre, 0)
    early = [pltpu.make_async_copy(a, b, out_sem.at[n]) for n, (a, b) in enumerate(
        ((x, x_out), (cosine, cos_out), (sine, sin_out), (actt, actt_out), (q, q_out), (k, k_out), (kt, kt_out), (v, v_out)))]
    for copy in early:
        copy.start()
    early[0].wait()

    def attend(i, carry):
        acc[...] = jnp.zeros_like(acc)
        stat[0] = jnp.full(stat.shape[1:], -1e30, jnp.float32)
        stat[1] = jnp.zeros(stat.shape[1:], jnp.float32)

        def block(j, masked, wide=1):
            key = k[pl.ds(j, wide)].reshape(wide * rows, dim)
            for h in range(heads):
                s = dot(key, q[i, :, h * dim:(h + 1) * dim], NT)
                c = SOFT_CAP * jnp.tanh(s * (1.0 / SOFT_CAP))
                if masked:
                    allowed = lax.broadcasted_iota(jnp.int32, s.shape, 0) <= lax.broadcasted_iota(jnp.int32, s.shape, 1)
                    c = jnp.where(allowed, c, -1e30)
                old = stat[0, h:h + 1, :]
                new = jnp.maximum(old, jnp.max(c, axis=0, keepdims=True))
                scale = jnp.exp(old - new)
                p = jnp.exp(c - new)
                stat[1, h:h + 1, :] = stat[1, h:h + 1, :] * scale + jnp.sum(p, axis=0, keepdims=True)
                stat[0, h:h + 1, :] = new
                p = bf(p)
                out_t = dot(vt[j], p[:rows])
                for n in range(1, wide):
                    out_t = out_t + dot(vt[j + n], p[n * rows:(n + 1) * rows])
                acc[h] = acc[h] * scale + out_t

        def body(j, carry):
            block(2 * j, False, 2)
            return carry

        lax.fori_loop(0, i // 2, body, 0)

        @pl.when(lax.rem(i, 2) == 1)
        def _():
            block(i - 1, False)

        block(i, True)
        lse_out[i] = stat[0] + jnp.log(stat[1])
        parts = []
        for h in range(heads):
            out_t = acc[h] / stat[1, h:h + 1, :]
            at(ot.at[h * dim:(h + 1) * dim], i, rows)[...] = bf(out_t)
            out = out_t.T
            of[i, :, h * dim:(h + 1) * dim] = out
            parts.append(bf(out))
        zb = bf(dot(jnp.concatenate(parts, axis=1), wo[...]))
        z[pl.ds(pl.multiple_of(i * rows, rows), rows), :] = zb
        zf = zb.astype(jnp.float32)
        post = bf(zf * inv_rms(zf) * (1.0 + gain_post[...]))
        x[i] = bf(x[i].astype(jnp.float32) + post.astype(jnp.float32))
        return carry

    lax.fori_loop(0, count, attend, 0)
    y_copy = pltpu.make_async_copy(x, y_out, out_sem.at[8])
    y_copy.start()
    dpost_out[...] = jnp.zeros_like(dpost_out)

    def mid(t, carry):
        j = lax.rem(me + count - distance(t, count), count)
        dy_move.wait_from(j)
        rws = pl.ds(pl.multiple_of(j * rows, rows), rows)
        dz, dgain = norm_grad(z[rws, :].astype(jnp.float32), gain_post[...], dy[j].astype(jnp.float32))
        dpost_out[...] += jnp.sum(dgain.reshape(rows // 8, 8, model), axis=0)
        dz = bf(dz)
        z[rws, :] = dz
        lane = lax.broadcasted_iota(jnp.int32, (rows, 128), 1)
        cols = jnp.zeros((rows, 128), jnp.float32)
        for h in range(heads):
            sl = slice(h * dim, (h + 1) * dim)
            doh = bf(dot(dz, wo[sl, :], NT))
            do[j, :, sl] = doh
            cols = jnp.where(lane == h, jnp.sum(doh.astype(jnp.float32) * of[j, :, sl], axis=-1, keepdims=True), cols)
        delta_out[j] = cols.T[:8, :]
        return carry

    lax.fori_loop(0, count, mid, 0)
    late = [pltpu.make_async_copy(dy, dy_out, out_sem.at[9]), pltpu.make_async_copy(do, do_out, out_sem.at[10])]
    for copy in late:
        copy.start()

    def put(h, slot):
        return pltpu.make_async_copy(dwo.at[slot], dwo_out.at[h], dwo_sem.at[slot])

    def weight(h, carry):
        slot = lax.rem(h, 2)

        @pl.when(h >= 2)
        def _():
            put(h - 2, slot).wait()

        dwo[slot] = dot(ot[pl.ds(pl.multiple_of(h * dim, dim), dim), :], z[...])
        put(h, slot).start()
        return carry

    lax.fori_loop(0, heads, weight, 0)
    for h in range(heads - 2, heads):
        put(h, h % 2).wait()
    for copy in early[1:] + [y_copy] + late:
        copy.wait()
    x_move.wait_sent()
    dy_move.wait_sent()


def front(count, heads, x_in, dy_in, angle, gain_pre, gain_post, wq, wk, wv, wo):
    bf16, f32 = jnp.bfloat16, jnp.float32
    _, rows, model = x_in.shape
    dim = wk.shape[1]
    width = heads * dim
    tokens = count * rows
    seq = lambda cols, dtype=bf16: ((count, rows, cols), dtype)
    kv = [seq(dim)] * 4
    hbm = pl.BlockSpec(memory_space=pl.ANY)
    vmem = pl.BlockSpec(memory_space=pltpu.VMEM)
    stat = ((count, 8, rows), f32)
    outs = [seq(model), seq(model), seq(dim // 2, f32), seq(dim // 2, f32), ((model, tokens), bf16), seq(width)] + kv[:3] + [
        seq(model), seq(width), ((heads, dim, model), f32), stat, stat, ((8, model), f32)]
    scratch = [seq(model), seq(model), (wq.shape, bf16), (wk.shape, bf16), (wv.shape, bf16), (wo.shape, bf16), seq(dim // 2, f32), seq(dim // 2, f32),
               ((model, tokens), bf16), seq(width)] + kv + [seq(width, f32), ((width, tokens), bf16), ((tokens, model), bf16), seq(width),
               ((2, dim, model), f32), ((heads, dim, rows), f32), ((2, 8, rows), f32)]
    sems = [count, count, count, count, 4, 11, 2]
    return pl.pallas_call(
        functools.partial(front_kernel, count, heads),
        name="front",
        in_specs=[hbm, hbm, vmem, vmem, vmem, hbm, hbm, hbm, hbm],
        out_specs=[hbm] * 12 + [vmem] * 3,
        out_shape=[jax.ShapeDtypeStruct(*o) for o in outs],
        scratch_shapes=[pltpu.VMEM(*s) for s in scratch] + [pltpu.SemaphoreType.DMA((n,)) for n in sems],
        compiler_params=pltpu.CompilerParams(collective_id=1, has_side_effects=True, vmem_limit_bytes=67000000),
        cost_estimate=pl.CostEstimate(flops=10 ** 10, bytes_accessed=8 * 2 ** 20, transcendentals=0),
    )(x_in, dy_in, angle, gain_pre, gain_post, wq, wk, wv, wo)


class SumAll:
    def __init__(self, total, out, slots, send, recv, keep, me):
        self.total, self.out, self.send, self.recv, self.keep = total, out, send, recv, keep
        self.from_core, self.from_first, self.from_second = slots
        core, chip = lax.rem(me, 2), me // 2
        self.core = core
        swap = chip + 1 - 2 * lax.rem(chip, 2)
        turn = lax.rem(chip + 3 + 2 * lax.rem(chip, 2), 4)
        low, high = lax.rem((chip + 1) // 2, 2), chip // 2
        self.sibling = me + 1 - 2 * core
        self.first = (swap * 2 + core, turn * 2 + core)
        self.second = (turn * 2 + core, swap * 2 + core)
        self.sub = (low, high)
        self.quarter = (high, low)
        self.base = (core * 8, core * 8 + 4)

    def move(self, start, blocks, target, at_block, sem, device, source=None):
        source = self.total if source is None else source
        return pltpu.make_async_remote_copy(
            src_ref=source.at[pl.ds(start, blocks)], dst_ref=target.at[pl.ds(at_block, blocks)], send_sem=self.send.at[sem],
            recv_sem=self.recv.at[sem], device_id={"cp": device}, device_id_type=MESH)

    def half(self):
        return self.move((1 - self.core) * 8, 8, self.from_core, 0, 0, self.sibling)

    def reduce_first(self, s):
        return self.move(self.base[s] + (1 - self.sub[s]) * 2, 2, self.from_first, 2 * s, 1 + s, self.first[s])

    def reduce_second(self, s):
        return self.move(self.base[s] + self.sub[s] * 2 + 1 - self.quarter[s], 1, self.from_second, s, 3 + s, self.second[s])

    def gather_second(self, s):
        at_block = self.base[s] + self.sub[s] * 2 + self.quarter[s]
        return self.move(at_block, 1, self.out, at_block, 5 + s, self.second[s])

    def keep_own(self, s):
        block = pl.ds(self.base[s] + self.sub[s] * 2 + self.quarter[s], 1)
        return pltpu.make_async_copy(self.total.at[block], self.out.at[block], self.keep.at[s])

    def gather_first(self, s):
        at_block = self.base[s] + self.sub[s] * 2
        return self.move(at_block, 2, self.out, at_block, 7 + s, self.first[s], self.out)

    def share_own(self, s):
        at_block = self.base[s] + self.sub[s] * 2
        return self.move(at_block, 2, self.out, at_block, 9 + s, self.sibling, self.out)

    def share_other(self, s):
        at_block = self.base[s] + (1 - self.sub[s]) * 2
        return self.move(at_block, 2, self.out, at_block, 11 + s, self.sibling, self.out)

    def add(self, start, source, at_block, blocks):
        def body(n, carry):
            self.total[start + n] = self.total[start + n] + source[at_block + n]
            return carry

        lax.fori_loop(0, blocks, body, 0)

    def begin(self):
        self.half().start()

    def finish_half(self):
        self.half().wait_recv()
        for s in range(2):
            self.add(self.base[s] + (1 - self.sub[s]) * 2, self.from_core, s * 4 + (1 - self.sub[s]) * 2, 2)
        for s in range(2):
            self.reduce_first(s).start()
        for s in range(2):
            self.add(self.base[s] + self.sub[s] * 2, self.from_core, s * 4 + self.sub[s] * 2, 2)

    def finish_first(self):
        for s in range(2):
            self.reduce_first(s).wait_recv()
            self.add(self.base[s] + self.sub[s] * 2, self.from_first, 2 * s, 2)
            self.reduce_second(s).start()

    def finish_second(self):
        for s in range(2):
            self.reduce_second(s).wait_recv()
            self.add(self.base[s] + self.sub[s] * 2 + self.quarter[s], self.from_second, s, 1)
            self.gather_second(s).start()
            self.keep_own(s).start()

    def finish_gather(self):
        for s in range(2):
            self.gather_second(s).wait_recv()
            self.keep_own(s).wait()
            self.gather_first(s).start()
            self.share_own(s).start()

    def finish_share(self):
        for s in range(2):
            self.gather_first(s).wait_recv()
            self.share_other(s).start()

    def end(self):
        for s in range(2):
            self.share_own(s).wait_recv()
            self.share_other(s).wait_recv()
        self.half().wait_send()
        for s in range(2):
            for step in (self.reduce_first, self.reduce_second, self.gather_second, self.gather_first, self.share_own, self.share_other):
                step(s).wait_send()


def back_kernel(count, heads, y_in, x_in, dy_in, q_in, do_in, k_in, kt_in, v_in, actt_in, cos_in, sin_in, dwo_in, wq_in, wk_in, wv_in,
                lse, delta, dpost, gain_pre,
                y_out, dx_out, dwo_out, dqkv_out, gains_out,
                x, dy, q, do, k, kt, v, actt, cosine, sine, wqkv, dqkv, dqt, dka, dva, dx, dpre, gains,
                wo_sum, wo_half, wo_first, wo_second, qkv_sum, qkv_half, qkv_first, qkv_second,
                y_send, y_recv, dx_send, dx_recv, gain_send, gain_recv, wo_send, wo_recv, qkv_send, qkv_recv, load_sem, piece_sem, wo_keep, qkv_keep):
    me = lax.axis_index("cp")
    rows, model = x.shape[1:]
    dim = k.shape[-1]
    width = heads * dim
    greet(me, count)
    wo_total = SumAll(wo_sum, dwo_out, (wo_half, wo_first, wo_second), wo_send, wo_recv, wo_keep, me)
    qkv_total = SumAll(qkv_sum, dqkv_out, (qkv_half, qkv_first, qkv_second), qkv_send, qkv_recv, qkv_keep, me)
    y_move = Exchange(y_in, y_out, y_send, y_recv, me, count)
    dx_move = Exchange(dx, dx_out, dx_send, dx_recv, me, count)
    order = [0] + near_first(count)

    def fetch(i, slot):
        return [pltpu.make_async_copy(a.at[i], b.at[slot], piece_sem.at[slot, n]) for n, (a, b) in enumerate(
            ((q_in, q), (do_in, do), (x_in, x), (dy_in, dy)))]

    loads = [pltpu.make_async_copy(a, b, load_sem.at[n]) for n, (a, b) in enumerate((
        (dwo_in, wo_sum), (k_in, k), (kt_in, kt), (v_in, v), (cos_in, cosine), (sin_in, sine),
        (wq_in, wqkv.at[:, 0:width]), (wk_in, wqkv.at[:, width:width + dim]), (wv_in, wqkv.at[:, width + dim:]), (actt_in, actt)))]
    for load in loads:
        load.start()
    for load in fetch(count - 1, 0):
        load.start()
    loads[0].wait()
    wo_total.begin()
    dka[...] = jnp.zeros_like(dka)
    dva[...] = jnp.zeros_like(dva)
    dpre[...] = jnp.zeros_like(dpre)
    for load in loads[1:]:
        load.wait()
    wo_total.finish_half()
    y_move.start(order[:4])

    def step(g, carry):
        i = count - 1 - g
        slot = lax.rem(g, 2)

        @pl.when(g < count - 1)
        def _():
            for load in fetch(i - 1, 1 - slot):
                load.start()

        for load in fetch(i, slot):
            load.wait()
        dqt[...] = jnp.zeros_like(dqt)

        def block(j, masked):
            key, key_t, val = k[j], kt[j], v[j]
            for h in range(heads):
                qh = q[slot, :, h * dim:(h + 1) * dim]
                doh = do[slot, :, h * dim:(h + 1) * dim]
                t = jnp.tanh(dot(key, qh, NT) * (1.0 / SOFT_CAP))
                p = jnp.exp(SOFT_CAP * t - lse[i, h:h + 1, :])
                if masked:
                    allowed = lax.broadcasted_iota(jnp.int32, t.shape, 0) <= lax.broadcasted_iota(jnp.int32, t.shape, 1)
                    p = jnp.where(allowed, p, 0.0)
                dp = dot(val, doh, NT)
                ds = bf(p * (dp - delta[i, h:h + 1, :]) * (1.0 - t * t))
                dva[j] += dot(bf(p), doh)
                dka[j] += dot(ds, qh)
                dqt[h] += dot(key_t, ds)

        def body(j, carry):
            block(j, False)
            return carry

        lax.fori_loop(0, i, body, 0)
        block(i, True)
        c, s = cosine[i], sine[i]
        rws = pl.ds(pl.multiple_of(i * rows, rows), rows)
        for h in range(heads):
            dqkv[rws, h * dim:(h + 1) * dim] = bf(rotate_back(dqt[h].T, c, s) * QUERY_SCALE ** -0.5)
        dqkv[rws, width:width + dim] = bf(rotate_back(dka[i], c, s))
        dqkv[rws, width + dim:] = bf(dva[i])
        da = dot(dqkv[rws, :], wqkv[...], NT)
        du, dgain = norm_grad(x[slot].astype(jnp.float32), gain_pre[...], da)
        dpre[...] += jnp.sum(dgain.reshape(rows // 8, 8, model), axis=0)
        dx[i] = bf(dy[slot].astype(jnp.float32) + du)

        @pl.when(g == 1)
        def _():
            wo_total.finish_first()
            y_move.start(order[4:6])

        @pl.when(g == 3)
        def _():
            wo_total.finish_second()
            y_move.start(order[6:])

        @pl.when(g == 5)
        def _():
            wo_total.finish_gather()

        return carry

    lax.fori_loop(0, count, step, 0)
    dx_move.start(order[-3:])
    part = qkv_sum.shape[1] * 4

    def weight(n, carry):
        at_block = lax.rem((1 - qkv_total.core) * 2 + n, 4)
        lhs = actt[pl.ds(pl.multiple_of(at_block * part, 16), part), :]
        qkv_sum[pl.ds(at_block * 4, 4)] = dot(lhs, dqkv[...]).reshape(4, part // 4, width + 2 * dim)

        @pl.when(n == 1)
        def _():
            qkv_total.begin()
            wo_total.finish_share()

        return carry

    lax.fori_loop(0, 4, weight, 0)
    gains[me] = jnp.concatenate([jnp.sum(dpre[...], axis=0, keepdims=True), jnp.sum(dpost[...], axis=0, keepdims=True), jnp.zeros((6, model), jnp.float32)], axis=0)
    qkv_total.finish_half()
    dx_move.start(order[:2])

    def send_gains(step):
        to = lax.rem(me + step, count)
        return pltpu.make_async_remote_copy(
            src_ref=gains.at[me], dst_ref=gains.at[me], send_sem=gain_send.at[to], recv_sem=gain_recv.at[me], device_id={"cp": to}, device_id_type=MESH)

    for n in range(1, count):
        send_gains(n).start()
    qkv_total.finish_first()
    dx_move.start(order[2:4])
    wo_total.end()
    for n in range(1, count):
        source = lax.rem(me + n, count)
        pltpu.make_async_copy(gains.at[source], gains.at[source], gain_recv.at[source]).wait()
    gains_out[...] = jnp.sum(gains[...], axis=0)
    qkv_total.finish_second()
    dx_move.start(order[4:-3])
    qkv_total.finish_gather()
    qkv_total.finish_share()
    qkv_total.end()
    for n in range(1, count):
        send_gains(n).wait_send()
    for source in range(count):
        dx_move.wait_from(source)
    dx_move.wait_sent()
    for source in range(count):
        y_move.wait_from(source)
    y_move.wait_sent()


def back(count, heads, y, x, dy, q, do, k, kt, v, actt, cosine, sine, dwo, wq, wk, wv, lse, delta, dpost, gain_pre):
    bf16, f32 = jnp.bfloat16, jnp.float32
    _, rows, model = x.shape
    dim = wk.shape[1]
    width = heads * dim
    wide = width + 2 * dim
    tokens = count * rows
    seq = lambda cols, dtype=bf16, n=count: ((n, rows, cols), dtype)
    blocks = lambda n, height, cols: ((n, height // 16, cols), f32)
    hbm = pl.BlockSpec(memory_space=pl.ANY)
    vmem = pl.BlockSpec(memory_space=pltpu.VMEM)
    outs = [seq(model), seq(model), blocks(16, width, model), blocks(16, model, wide), ((8, model), f32)]
    scratch = [seq(model, n=2), seq(model, n=2), seq(width, n=2), seq(width, n=2), seq(dim), seq(dim), seq(dim), (actt.shape, bf16),
               seq(dim // 2, f32), seq(dim // 2, f32), ((model, wide), bf16), ((tokens, wide), bf16), ((heads, dim, rows), f32),
               seq(dim, f32), seq(dim, f32), seq(model), ((8, model), f32), ((count, 8, model), f32)]
    scratch += [blocks(n, width, model) for n in (16, 8, 4, 2)] + [blocks(n, model, wide) for n in (16, 8, 4, 2)]
    sems = [(count,)] * 6 + [(13,)] * 4 + [(10,), (2, 4), (2,), (2,)]
    return pl.pallas_call(
        functools.partial(back_kernel, count, heads),
        name="back",
        in_specs=[hbm] * 15 + [vmem] * 4,
        out_specs=[hbm] * 4 + [vmem],
        out_shape=[jax.ShapeDtypeStruct(*o) for o in outs],
        scratch_shapes=[pltpu.VMEM(*s) for s in scratch] + [pltpu.SemaphoreType.DMA(n) for n in sems],
        compiler_params=pltpu.CompilerParams(collective_id=2, has_side_effects=True, vmem_limit_bytes=67000000),
        cost_estimate=pl.CostEstimate(flops=10 ** 10, bytes_accessed=8 * 2 ** 20, transcendentals=0),
    )(y, x, dy, q, do, k, kt, v, actt, cosine, sine, dwo.reshape(16, width // 16, model), wq, wk, wv, lse, delta, dpost, gain_pre)


def finish_kernel(y, dx, dwo, y_out, dx_out, dwo_out):
    y_out[...] = y[...]
    dx_out[...] = dx[...]
    dwo_out[...] = dwo[...]


def finish(count, y, dx, dwo):
    dwo = dwo.reshape(count, -1, dwo.shape[-1])
    specs = [pl.BlockSpec((1,) + a.shape[1:], lambda i: (i, 0, 0)) for a in (y, dx, dwo)]
    return pl.pallas_call(
        finish_kernel,
        name="finish",
        grid=(count,),
        in_specs=specs,
        out_specs=specs,
        out_shape=[jax.ShapeDtypeStruct(a.shape, a.dtype) for a in (y, dx, dwo)],
        compiler_params=pltpu.CompilerParams(dimension_semantics=("arbitrary",)),
        cost_estimate=pl.CostEstimate(flops=10 ** 8, bytes_accessed=8 * 2 ** 20, transcendentals=0),
    )(y, dx, dwo)


def solution(mesh):
    count = mesh.shape["cp"]

    def local_step(x_in, positions, dy_out, w_query, w_key, w_value, w_out, w_pre, w_post):
        model = x_in.shape[-1]
        heads, dim = w_query.shape[1], w_query.shape[2]
        width = heads * dim
        f32 = jnp.float32
        wq = w_query.reshape(model, width)
        wk = w_key.reshape(model, dim)
        wv = w_value.reshape(model, dim)
        wo = w_out.reshape(width, model)
        gain_pre = w_pre.reshape(1, model)
        gain_post = w_post.reshape(1, model)

        pos = lax.all_to_all(positions, "cp", 0, 0, tiled=True)
        inv_freq = ROPE_BASE ** (jnp.arange(dim // 2, dtype=f32) * (-2.0 / dim))
        angle = pos.astype(f32)[:, :, None] * inv_freq
        x, dy, cosine, sine, actt, q, k, kt, v, y, do, dwo, lse, delta, dpost = front(
            count, heads, x_in, dy_out, angle, gain_pre, gain_post, wq, wk, wv, wo)
        y_out, dx_in, dwo, dqkv, gains = back(
            count, heads, y, x, dy, q, do, k, kt, v, actt, cosine, sine, dwo, wq, wk, wv, lse, delta, dpost, gain_pre)
        y_out, dx_in, dwo = finish(count, y_out, dx_in, dwo)
        width = heads * dim
        dqkv = dqkv.reshape(model, width + 2 * dim)
        return (y_out, dx_in, dqkv[:, :width].reshape(model, heads, dim), dqkv[:, None, width:width + dim], dqkv[:, None, width + dim:],
                dwo.reshape(heads, dim, model), gains[0], gains[1])

    seq_spec = P("dp", "cp", None)
    in_specs = (seq_spec, P("dp", "cp"), seq_spec, P(), P(), P(), P(), P(), P())
    out_specs = (seq_spec, seq_spec, P("dp", None, None), P("dp", None, None), P("dp", None, None), P("dp", None, None), P("dp"), P("dp"))
    return jax.shard_map(local_step, mesh=mesh, in_specs=in_specs, out_specs=out_specs, check_vma=False)
```
